128 devices in a mesh: gx: 8 (over z, core), gy: 16 (over x, y).
Axes of the slice: x: 4, y: 4, z: 4, core: 2. Of those that a mesh axis runs over, the one named last changes fastest.
Arguments:
- atm_members: float32 [8, 16, 80, 12, 128], P('gx', 'gy'), may hold values from -6 to 6
- ocean_members: bfloat16 [8, 16, 80, 1024], P('gx', 'gy'), may hold values from -6 to 6
- remap_weights: bfloat16 [8, 16, 4, 1024, 128], P('gx', 'gy'), may hold values from -0.09375 to 0.09375
- pair_src: int32 [8, 16, 4], P('gx', 'gy'), may hold values from 0 to 127, as said below
- obs_cell: int32 [8, 16, 64], P('gx', 'gy'), may hold values from 0 to 127
- obs_value: float32 [8, 16, 64], P('gx', 'gy'), may hold values from -8 to 8
- obs_error: float32 [8, 16, 64], P('gx', 'gy'), may hold values from 2 to 16
- obs_live: int32 [8, 16, 64], P('gx', 'gy'), may hold values from 0 to 1, as said below
- obs_order: int32 [8, 16, 64], P('gx', 'gy'), may hold values from 0 to 63, each once within a row
Outputs:
- post_mean: float32 [8, 16, 13, 128], P('gx', 'gy')
- post_anom: float32 [8, 16, 80, 13, 128], P('gx', 'gy')
The draws below stay inside these ranges and needn't reach their ends.
Inputs may be any that keep to these rules, and one draw needn't show every extreme that they name: `pair_src`: for atmosphere tile (i, j) the 4 numbers are distinct, each a * 16 + b with |a - i| <= 1 and |b - j| <= 1. `obs_live`: the live slots of a tile are its first ones, between 8 and 64 of them; some tile has all slots live. `obs_order`: each tile's last dimension is a permutation of its slots.
All inputs are finite; a program needn't handle non-finite values.
Results may differ from the reference program's by a relative error of at most 0.0003.
Values may be sent and summed in bfloat16 or wider, within the bound.
A program may use at most 64 MiB of HBM per device.

```python
import math
import jax
import jax.numpy as jnp
from jax import lax

MEM = 80
AX = 8
AY = 16
OCN_DEV = 1024
OB = 32
NB = 2
K = 4
FIELDS = 12
COMP = 13
CELLS = 128
RAD = 2
OBS_DEV = 64
TILES_X = 8
TILES_Y = 16


def draw_pair_src(key, part):
    tile_x = jnp.arange(TILES_X, dtype=jnp.int32)[:, None, None]
    tile_y = jnp.arange(TILES_Y, dtype=jnp.int32)[None, :, None]
    candidate = jnp.arange(9, dtype=jnp.int32)[None, None, :]
    source_x = tile_x + candidate // 3 - 1
    source_y = tile_y + candidate % 3 - 1
    scores = jax.random.randint(jax.random.fold_in(key, 11), (TILES_X, TILES_Y, 9), 0, 1 << 20)
    scores = scores * 9 + candidate
    outside = (source_x < 0) | (source_x >= TILES_X) | (source_y < 0) | (source_y >= TILES_Y)
    scores = jnp.where(outside, scores + (1 << 29), scores)
    ranking = jnp.argsort(scores, axis=-1)[..., :K]
    linear = source_x * TILES_Y + source_y
    return jnp.take_along_axis(linear, ranking, axis=-1).astype(jnp.int32)


def draw_obs_live(key, part):
    threshold = jax.random.randint(jax.random.fold_in(key, 21), (TILES_X, TILES_Y), OBS_DEV // 8, OBS_DEV + 1)
    chosen_tile = jax.random.randint(jax.random.fold_in(key, 22), (), 0, TILES_X * TILES_Y)
    tile_number = jnp.arange(TILES_X * TILES_Y, dtype=jnp.int32).reshape(TILES_X, TILES_Y)
    threshold = jnp.where(tile_number == chosen_tile, OBS_DEV, threshold)
    slot_number = jnp.arange(OBS_DEV, dtype=jnp.int32)
    return (slot_number[None, None, :] < threshold[:, :, None]).astype(jnp.int32)


def plant(values, rng, smallest, top_value):
    longest = values.shape.index(max(values.shape))
    spots = []
    for shift in (0, 1):
        where = [jax.random.randint(jax.random.fold_in(rng, axis), (), 0, length) for axis, length in enumerate(values.shape)]
        where[longest] = (where[longest] + shift) % values.shape[longest]
        spots.append(tuple(where))
    return values.at[spots[0]].set(smallest).at[spots[1]].set(top_value)


def levels(key, shape, pieces, smallest, high):
    level, own = 1.0, jax.random.fold_in(key, 6)
    for axis_at, shards_of in pieces:
        heights = jnp.exp(jax.random.uniform(jax.random.fold_in(own, axis_at), (shards_of,), jnp.float32, smallest / len(pieces), high / len(pieces)))
        level = level * jnp.repeat(heights, shape[axis_at] // shards_of).reshape([-1 if axis == axis_at else 1 for axis in range(len(shape))])
    return level


def centred(rng, shape, spread, limit, pieces=(), held_as=jnp.bfloat16):
    values = spread * jax.random.normal(rng, shape, jnp.float32)
    if pieces:
        values = values * levels(rng, shape, pieces, -0.22, 0.18)
    return jnp.clip(values, -limit, limit).astype(held_as)


def setup_inputs(seed: int = 0) -> dict:
    splits = jax.random.split(jax.random.key(seed), 10)
    atm_members = centred(splits[0], (TILES_X, TILES_Y, MEM, FIELDS, CELLS), 1.0, 6.0, ((0, 8), (1, 16)), jnp.float32)
    ocean_members = centred(splits[1], (TILES_X, TILES_Y, MEM, OCN_DEV), 1.0, 6.0, ((0, 8), (1, 16)))
    remap_weights = centred(splits[2], (TILES_X, TILES_Y, K, OCN_DEV, CELLS), (K * OCN_DEV) ** -0.5, 0.09375, ((0, 8), (1, 16)))
    pair_src = draw_pair_src(jax.random.fold_in(splits[9], 71), 0)
    obs_cell = plant(jax.random.randint(splits[4], (TILES_X, TILES_Y, OBS_DEV), 0, CELLS), jax.random.fold_in(splits[4], 1), 0, CELLS - 1).astype(jnp.int32)
    obs_value = centred(splits[5], (TILES_X, TILES_Y, OBS_DEV), 1.5, 8.0, ((0, 8), (1, 16)), jnp.float32)
    obs_error = jnp.clip(jnp.exp(math.log(16.0) - 2.0794415 * jax.random.uniform(splits[6], (TILES_X, TILES_Y, OBS_DEV), jnp.float32) ** levels(splits[6], (TILES_X, TILES_Y, OBS_DEV), ((0, 8), (1, 16)), -0.2, 0.2)), 2.0, 16.0)
    obs_live = draw_obs_live(jax.random.fold_in(splits[9], 71), 0)
    obs_order = jax.vmap(lambda own: jax.random.permutation(own, OBS_DEV))(jax.random.split(splits[8], TILES_X * TILES_Y)).reshape((TILES_X, TILES_Y, OBS_DEV)).astype(jnp.int32)
    return {"atm_members": atm_members, "ocean_members": ocean_members, "remap_weights": remap_weights, "pair_src": pair_src, "obs_cell": obs_cell, "obs_value": obs_value, "obs_error": obs_error, "obs_live": obs_live, "obs_order": obs_order}


exact_mode = lax.Precision.HIGHEST

def update_group(packets, anomaly, ens_mean, base_x, base_y):
    members = anomaly.shape[0]
    components = anomaly.shape[1]
    cell_count = anomaly.shape[2]
    observed = jnp.transpose(packets[:, :members, :], (1, 0, 2)).reshape(members, -1)
    innovation = packets[:, members, :].reshape(-1)
    errors = packets[:, members + 1, :].reshape(-1)
    obs_x = packets[:, members + 2, :].reshape(-1)
    obs_y = packets[:, members + 3, :].reshape(-1)
    live = packets[:, members + 4, :].reshape(-1)
    variance = lax.optimization_barrier(jnp.sum(observed * observed, axis=0)) / (members - 1)
    denominator = variance + errors + (1.0 - live)
    weighting = live / denominator
    damping = 1.0 / (1.0 + jnp.sqrt(errors / denominator))
    cell_index = jnp.arange(cell_count, dtype=jnp.int32)
    cell_x = (base_x + cell_index // AY).astype(jnp.float32)
    cell_y = (base_y + cell_index % AY).astype(jnp.float32)
    distance = (obs_x[:, None] - cell_x[None, :]) ** 2 + (obs_y[:, None] - cell_y[None, :]) ** 2
    taper = jnp.maximum(1.0 - distance / float(RAD * RAD), 0.0) ** 2
    flat_anomaly = anomaly.reshape(members, components * cell_count)
    covariance = jnp.dot(observed.T, flat_anomaly, precision=exact_mode, preferred_element_type=jnp.float32) / (members - 1)
    gain = covariance.reshape(-1, components, cell_count) * (taper * weighting[:, None])[:, None, :]
    gain = gain.reshape(-1, components * cell_count)
    mean_step = jnp.dot(innovation[None, :], gain, precision=exact_mode, preferred_element_type=jnp.float32)
    anomaly_step = jnp.dot(observed * damping[None, :], gain, precision=exact_mode, preferred_element_type=jnp.float32)
    return (mean_step.reshape(components, cell_count), anomaly_step.reshape(members, components, cell_count))

def reference(atm_members, ocean_members, remap_weights, pair_src, obs_cell, obs_value, obs_error, obs_live, obs_order):
    tiles = TILES_X * TILES_Y
    ocean_flat = ocean_members.reshape(tiles, MEM, OCN_DEV)

    def remap_one(inputs):
        weights, sources = inputs
        chosen = ocean_flat[sources]
        stacked = jnp.transpose(chosen, (1, 0, 2)).reshape(MEM, K * OCN_DEV)
        return jnp.dot(stacked, weights.reshape(K * OCN_DEV, CELLS), preferred_element_type=jnp.float32)
    surface = lax.map(remap_one, (remap_weights.reshape(tiles, K, OCN_DEV, CELLS), pair_src.reshape(tiles, K).astype(jnp.int32)))
    state = jnp.concatenate([atm_members.reshape(tiles, MEM, FIELDS, CELLS), surface[:, :, None, :]], axis=2)
    ens_mean = lax.optimization_barrier(jnp.sum(state, axis=1)) / MEM
    anomaly = state - ens_mean[:, None]
    ens_mean = ens_mean.reshape(TILES_X, TILES_Y, COMP, CELLS)
    anomaly = anomaly.reshape(TILES_X, TILES_Y, MEM, COMP, CELLS)
    tile_x = jnp.broadcast_to(jnp.arange(TILES_X, dtype=jnp.int32)[:, None], (TILES_X, TILES_Y))
    tile_y = jnp.broadcast_to(jnp.arange(TILES_Y, dtype=jnp.int32)[None, :], (TILES_X, TILES_Y))
    base_x = tile_x * AX
    base_y = tile_y * AY
    for batch_index in range(NB):
        obs_slots = obs_order[:, :, batch_index * OB:(batch_index + 1) * OB].astype(jnp.int32)
        obs_cells = jnp.take_along_axis(obs_cell.astype(jnp.int32), obs_slots, axis=2)
        values = jnp.take_along_axis(obs_value, obs_slots, axis=2)
        errors = jnp.take_along_axis(obs_error, obs_slots, axis=2)
        live = jnp.take_along_axis(obs_live, obs_slots, axis=2).astype(jnp.float32)
        observed = jnp.take_along_axis(anomaly[:, :, :, FIELDS, :], obs_cells[:, :, None, :], axis=3)
        predicted = jnp.take_along_axis(ens_mean[:, :, FIELDS, :], obs_cells, axis=2)
        pos_x = (base_x[:, :, None] + obs_cells // AY).astype(jnp.float32)
        pos_y = (base_y[:, :, None] + obs_cells % AY).astype(jnp.float32)
        extras = jnp.stack([values - predicted, errors, pos_x, pos_y, live], axis=2)
        packet = jnp.concatenate([observed, extras], axis=2)
        padded = jnp.pad(packet, ((1, 1), (1, 1), (0, 0), (0, 0)))
        beside_all = jnp.stack([padded[row_shift:row_shift + TILES_X, col_shift:col_shift + TILES_Y] for row_shift in range(3) for col_shift in range(3)], axis=2)

        def one_tile(inputs):
            packets, tile_anomaly, tile_mean, anchor_x, anchor_y = inputs
            mean_step, anomaly_step = update_group(packets, tile_anomaly, tile_mean, anchor_x, anchor_y)
            return (tile_mean + mean_step, tile_anomaly - anomaly_step)
        new_mean, new_anomaly = lax.map(one_tile, (beside_all.reshape(tiles, 9, MEM + 5, OB), anomaly.reshape(tiles, MEM, COMP, CELLS), ens_mean.reshape(tiles, COMP, CELLS), base_x.reshape(tiles), base_y.reshape(tiles)))
        ens_mean = new_mean.reshape(TILES_X, TILES_Y, COMP, CELLS)
        anomaly = new_anomaly.reshape(TILES_X, TILES_Y, MEM, COMP, CELLS)
    return (ens_mean, anomaly)
```

```python
import functools

import jax
import jax.numpy as jnp
from jax import lax
from jax.experimental import pallas as pl
from jax.experimental.pallas import tpu as pltpu
from jax.sharding import PartitionSpec as P

MEM = 80
AX = 8
AY = 16
OCN_DEV = 1024
OB = 32
NB = 2
K = 4
FIELDS = 12
COMP = 13
CELLS = 128
OBS = 64
ROWS = 88
GROUPS = 11
CHUNKS = 4
CW = OCN_DEV // CHUNKS

MESH = pl.DeviceIdType.MESH
NEAR = [(dx, dy) for dx in (-1, 0, 1) for dy in (-1, 0, 1)]
AROUND = [d for d in NEAR if d != (0, 0)]


def slot(dx, dy):
    return (dx + 1) * 3 + dy + 1


def roll(x, shift):
    shift = shift % CELLS
    return x if shift == 0 else pltpu.roll(x, shift, 1)


def exchange_kernel(
    src,
    ocean,
    weights,
    cell,
    value,
    error,
    live,
    order,
    f_out,
    meta_out,
    oce,
    wv,
    acc,
    meta,
    meta_in,
    pack_y,
    pack_x,
    in_w,
    in_e,
    in_n,
    in_s,
    local_sem,
    oce_send,
    oce_recv,
    relay_send,
    meta_send,
    meta_recv,
    halo_send,
    halo_recv,
):
    i = lax.axis_index("gx")
    j = lax.axis_index("gy")
    nx = lax.axis_size("gx")
    ny = lax.axis_size("gy")

    def has(dx, dy):
        cond = None
        for pos, step, count in ((i, dx, nx), (j, dy, ny)):
            if step:
                ok = (pos > 0) if step < 0 else (pos < count - 1)
                cond = ok if cond is None else jnp.logical_and(cond, ok)
        return cond

    def when(dx, dy):
        return pl.when(has(dx, dy))

    def device(dx, dy):
        return (i + dx, j + dy)

    barrier = pltpu.get_barrier_semaphore()
    for dx, dy in AROUND:

        @when(dx, dy)
        def _():
            pl.semaphore_signal(
                barrier, inc=1, device_id=device(dx, dy), device_id_type=MESH
            )

    own_load = [
        pltpu.make_async_copy(
            ocean.at[:, pl.ds(c * CW, CW)], oce.at[4, c], local_sem.at[c]
        )
        for c in range(CHUNKS)
    ]
    for copy in own_load:
        copy.start()
    w_load = pltpu.make_async_copy(weights, wv, local_sem.at[CHUNKS])
    w_load.start()

    lane = lax.broadcasted_iota(jnp.int32, (OBS, OBS), 0)
    perm = jnp.where(lane == order[...], 1.0, 0.0)
    rows = [
        cell[...].astype(jnp.float32),
        value[...],
        error[...],
        live[...].astype(jnp.float32),
    ]
    stacked = jnp.concatenate(rows + [jnp.zeros((4, OBS), jnp.float32)], axis=0)
    ordered = jnp.dot(
        stacked,
        perm,
        precision=lax.Precision.HIGHEST,
        preferred_element_type=jnp.float32,
    )
    meta[...] = jnp.concatenate([ordered, jnp.zeros((8, CELLS - OBS), jnp.float32)], axis=1)

    xs = 1 + jnp.where(jnp.logical_and(i > 0, i < nx - 1), 1, 0)
    ys = 1 + jnp.where(jnp.logical_and(j > 0, j < ny - 1), 1, 0)
    pl.semaphore_wait(barrier, (xs + 1) * (ys + 1) - 1)

    def ocean_copy(c, dx, dy):
        return pltpu.make_async_remote_copy(
            src_ref=oce.at[4, c],
            dst_ref=oce.at[slot(-dx, -dy), c],
            send_sem=oce_send.at[slot(dx, dy), c],
            recv_sem=oce_recv.at[slot(-dx, -dy), c],
            device_id=device(dx, dy),
            device_id_type=MESH,
        )

    def relay_copy(c, dx, dy):
        return pltpu.make_async_remote_copy(
            src_ref=oce.at[slot(0, dy), c],
            dst_ref=oce.at[slot(-dx, dy), c],
            send_sem=relay_send.at[slot(dx, dy), c],
            recv_sem=oce_recv.at[slot(-dx, dy), c],
            device_id=device(dx, 0),
            device_id_type=MESH,
        )

    def meta_copy(dx, dy):
        return pltpu.make_async_remote_copy(
            src_ref=meta,
            dst_ref=meta_in.at[slot(-dx, -dy)],
            send_sem=meta_send.at[slot(dx, dy)],
            recv_sem=meta_recv.at[slot(-dx, -dy)],
            device_id=device(dx, dy),
            device_id_type=MESH,
        )

    for c in range(CHUNKS):
        own_load[c].wait()
        for dx, dy in ((0, -1), (0, 1), (-1, 0), (1, 0)):

            @when(dx, dy)
            def _():
                ocean_copy(c, dx, dy).start()

    for dx, dy in AROUND:

        @when(dx, dy)
        def _():
            meta_copy(dx, dy).start()

    positions = [
        (src[0, k] // ny - i + 1) * 3 + (src[0, k] % ny - j + 1) for k in range(K)
    ]

    def product(p, c):
        which = jnp.int32(0)
        valid = positions[0] == p
        for k in range(1, K):
            which = jnp.where(positions[k] == p, k, which)
            valid = jnp.logical_or(valid, positions[k] == p)
        part = jnp.dot(
            oce[p, c],
            wv[which, pl.ds(c * CW, CW), :],
            preferred_element_type=jnp.float32,
        )
        return jnp.where(valid, part, 0.0)

    w_load.wait()
    total = product(4, 0)
    for c in range(1, CHUNKS):
        total = total + product(4, c)
    acc[...] = total

    for c in range(CHUNKS):
        for dy in (-1, 1):

            @when(0, dy)
            def _():
                ocean_copy(c, 0, -dy).wait_recv()
                for dx in (-1, 1):

                    @when(dx, 0)
                    def _():
                        relay_copy(c, dx, dy).start()

        for dx, dy in ((-1, 0), (1, 0)):

            @when(dx, dy)
            def _():
                ocean_copy(c, -dx, -dy).wait_recv()
                acc[...] += product(slot(dx, dy), c)

        for dx, dy in ((0, -1), (0, 1)):

            @when(dx, dy)
            def _():
                acc[...] += product(slot(dx, dy), c)

    for dx, dy in AROUND:

        @when(dx, dy)
        def _():
            meta_copy(-dx, -dy).wait_recv()

    blocks = []
    for dx, dy in NEAR:
        if (dx, dy) == (0, 0):
            blocks.append(meta[...])
        else:
            blocks.append(jnp.where(has(dx, dy), meta_in[slot(dx, dy)], 0.0))
    blocks.append(jnp.zeros((CELLS - 72, CELLS), jnp.float32))
    columns = jnp.concatenate(blocks, axis=0).T
    meta_out[...] = columns[:OBS, :]

    for c in range(CHUNKS):
        for dx, dy in ((-1, -1), (-1, 1), (1, -1), (1, 1)):

            @when(dx, dy)
            def _():
                relay_copy(c, -dx, dy).wait_recv()
                acc[...] += product(slot(dx, dy), c)

    sst = acc[...]
    mean = jnp.sum(sst, axis=0, keepdims=True) / MEM
    anomaly = sst - mean
    pieces = [anomaly[8 * g : 8 * g + 8] for g in range(MEM // 8)]
    head = lax.broadcasted_iota(jnp.int32, (8, CELLS), 0) == 0
    pieces.append(jnp.where(head, mean, 0.0))
    lane8 = lax.broadcasted_iota(jnp.int32, (8, CELLS), 1)
    pair = (lane8 % AY) // 2
    quarter = lane8 // 32

    for block in range(2):
        west = jnp.zeros((8, CELLS), jnp.float32)
        east = west
        for g in range(8 * block, min(8 * block + 8, GROUPS)):
            s = g % 8
            west = jnp.where(pair == s, roll(pieces[g], 2 * s), west)
            east = jnp.where(pair == 7 - s, roll(pieces[g], -2 * s), east)
        pack_y[0, 8 * block : 8 * block + 8, :] = west
        pack_y[1, 8 * block : 8 * block + 8, :] = east
    for block in range(3):
        north = jnp.zeros((8, CELLS), jnp.float32)
        south = north
        for g in range(4 * block, min(4 * block + 4, GROUPS)):
            s = g % 4
            north = jnp.where(quarter == s, roll(pieces[g], 32 * s), north)
            south = jnp.where(quarter == 3 - s, roll(pieces[g], -32 * s), south)
        pack_x[0, 8 * block : 8 * block + 8, :] = north
        pack_x[1, 8 * block : 8 * block + 8, :] = south

    def halo_copy(dx, dy):
        if dy < 0:
            source, target = pack_y.at[0], in_w.at[1 - dx]
        elif dy > 0:
            source, target = pack_y.at[1], in_e.at[1 - dx]
        elif dx < 0:
            source, target = pack_x.at[0], in_n
        else:
            source, target = pack_x.at[1], in_s
        return pltpu.make_async_remote_copy(
            src_ref=source,
            dst_ref=target,
            send_sem=halo_send.at[slot(dx, dy)],
            recv_sem=halo_recv.at[slot(-dx, -dy)],
            device_id=device(dx, dy),
            device_id_type=MESH,
        )

    f_out[0, :MEM, :] = anomaly
    f_out[0, MEM:, :] = pieces[-1]

    for dx, dy in AROUND[::-1]:

        @when(dx, dy)
        def _():
            halo_copy(dx, dy).start()

    for c in range(CHUNKS):
        for dx, dy in ((0, -1), (0, 1), (-1, 0), (1, 0)):

            @when(dx, dy)
            def _():
                ocean_copy(c, dx, dy).wait_send()

        for dy in (-1, 1):
            for dx in (-1, 1):

                @when(dx, dy)
                def _():
                    relay_copy(c, dx, dy).wait_send()

    for dx, dy in AROUND:

        @when(dx, dy)
        def _():
            meta_copy(dx, dy).wait_send()

    for dx, dy in AROUND:

        @when(dx, dy)
        def _():
            halo_copy(-dx, -dy).wait_recv()

    low_y = (lane8 % AY) < 8
    low_x = lane8 < 64
    zero = jnp.zeros((8, CELLS), jnp.float32)

    def present(ref, dx, dy):
        return jnp.where(has(dx, dy), ref[...], 0.0)

    north = present(in_n, 1, 0)
    south = present(in_s, -1, 0)
    west = present(in_w.at[1], 0, 1)
    east = present(in_e.at[1], 0, -1)
    low16 = lax.broadcasted_iota(jnp.int32, (16, CELLS), 1) < 64
    west_c = jnp.where(low16, present(in_w.at[2], 1, 1), present(in_w.at[0], -1, 1))
    east_c = jnp.where(low16, present(in_e.at[2], 1, -1), present(in_e.at[0], -1, -1))
    for g in range(GROUPS):
        at = pl.ds(8 * g, 8)
        b, s = g // 4, g % 4
        f_out[1, at, :] = jnp.where(
            low_x,
            roll(north[8 * b : 8 * b + 8], -32 * s),
            roll(south[8 * b : 8 * b + 8], 32 * s),
        )
        b, s = g // 8, g % 8
        for place, w, e in ((2, west, east), (3, west_c, east_c)):
            f_out[place, at, :] = jnp.where(
                low_y,
                roll(w[8 * b : 8 * b + 8], -2 * s),
                roll(e[8 * b : 8 * b + 8], 2 * s),
            )

    for dx, dy in AROUND:

        @when(dx, dy)
        def _():
            halo_copy(dx, dy).wait_send()


def update_kernel(
    f_in, meta, atm, mean_out, anom_out, state, fields, shifted, scaled, sst_mean
):
    lane8 = lax.broadcasted_iota(jnp.int32, (8, CELLS), 1)
    y8 = lane8 % AY
    first_y, last_y = y8 == 0, y8 == AY - 1
    first_x, last_x = lane8 < AY, lane8 >= CELLS - AY

    def shift_all(blocks, wanted):
        out = {}
        turned = {}
        for f in range(4):
            if any((f ^ a) in wanted for a in (0, 1)):
                other = blocks[f ^ 2]
                turned[f, 0] = blocks[f]
                turned[f, 1] = jnp.where(last_y, roll(other, 15), roll(blocks[f], -1))
                turned[f, -1] = jnp.where(first_y, roll(other, -15), roll(blocks[f], 1))
        for f in wanted:
            for dy in (-1, 0, 1):
                own, other = turned[f, dy], turned[f ^ 1, dy]
                out[f, 0, dy] = own
                out[f, 1, dy] = roll(jnp.where(first_x, other, own), -AY)
                out[f, -1, dy] = roll(jnp.where(last_x, other, own), AY)
        return out

    total = jnp.zeros((FIELDS, CELLS), jnp.float32)

    def add_member(m, total):
        return total + atm[m]

    total = lax.fori_loop(0, MEM, add_member, total, unroll=8)
    field_mean = total / MEM

    def put_member(m, carry):
        fields[m, :FIELDS, :] = atm[m] - field_mean
        fields[m, FIELDS:COMP, :] = f_in[0, pl.ds(m, 1), :]
        return carry

    lax.fori_loop(0, MEM, put_member, 0, unroll=8)
    fields[MEM, :FIELDS, :] = field_mean
    fields[MEM, FIELDS:COMP, :] = f_in[0, MEM : MEM + 1, :]

    row32 = lax.broadcasted_iota(jnp.int32, (OB, CELLS), 1)
    row1 = lax.broadcasted_iota(jnp.int32, (1, CELLS), 1)
    low_y1 = (row1 % AY) < 8
    low_x1 = row1 < 64

    for batch in range(NB):
        source = f_in if batch == 0 else state
        wanted = (0, 1, 2, 3) if batch == 0 else (0,)

        variance = [
            jnp.sum(source[f, :MEM, :] * source[f, :MEM, :], axis=0, keepdims=True)
            / (MEM - 1)
            for f in range(4)
        ]

        def observations(f, dx, dy):
            at = 8 * slot(dx, dy)
            rows = slice(batch * OB, (batch + 1) * OB)
            cells = meta[rows, at : at + 1]
            values = meta[rows, at + 1 : at + 2]
            errors = meta[rows, at + 2 : at + 3]
            alive = meta[rows, at + 3 : at + 4]
            denominator = variance[f] + errors + (1.0 - alive)
            weighting = alive / denominator
            damping = 1.0 / (1.0 + jnp.sqrt(errors / denominator))
            weighting = jnp.where(cells == row32.astype(jnp.float32), weighting, 0.0)
            innovation = values - source[f, MEM : MEM + 1, :]
            alpha = jnp.sum(weighting * innovation, axis=0, keepdims=True)
            beta = jnp.sum(weighting * damping, axis=0, keepdims=True)
            return jnp.concatenate([beta, alpha], axis=0)

        pick = jnp.where
        sums = [
            observations(0, 0, 0),
            pick(low_x1, observations(1, 1, 0), observations(1, -1, 0)),
            pick(low_y1, observations(2, 0, 1), observations(2, 0, -1)),
            pick(
                low_y1,
                pick(low_x1, observations(3, 1, 1), observations(3, -1, 1)),
                pick(low_x1, observations(3, 1, -1), observations(3, -1, -1)),
            ),
        ]
        pad = jnp.zeros((6, CELLS), jnp.float32)
        factors = shift_all([jnp.concatenate([s, pad], axis=0) for s in sums], wanted)

        for g in range(MEM // 8):
            at = slice(8 * g, 8 * g + 8)
            moved = shift_all([source[f, at, :] for f in range(4)], wanted)
            for f in wanted:
                for dx, dy in NEAR:
                    shifted[f, slot(dx, dy), at, :] = moved[f, dx, dy]

        def taper(dx, dy):
            return max(1.0 - (dx * dx + dy * dy) / 4.0, 0.0) ** 2 / (MEM - 1)

        if batch + 1 < NB:
            for f in wanted:
                own = source[f, :MEM, :]
                new = own
                mean = source[f, MEM : MEM + 1, :]
                for dx, dy in NEAR:
                    h = shifted[f, slot(dx, dy), :MEM, :]
                    gain = jnp.sum(h * own, axis=0, keepdims=True) * taper(dx, dy)
                    beta = factors[f, dx, dy][0:1]
                    alpha = factors[f, dx, dy][1:2]
                    new = new - h * (beta * gain)
                    mean = mean + alpha * gain
                state[f, :MEM, :] = new
                state[f, MEM : MEM + 1, :] = mean

        for dx, dy in NEAR:
            d = slot(dx, dy)
            beta = factors[0, dx, dy][0:1]
            scaled[d, :MEM, :] = shifted[0, d, :MEM, :] * beta
            scaled[d, MEM : MEM + 1, :] = -factors[0, dx, dy][1:2]

        def accumulate(m, sums):
            block = fields[m]
            return tuple(
                s + shifted[0, d, pl.ds(m, 1), :] * block for d, s in enumerate(sums)
            )

        gains = lax.fori_loop(
            0,
            MEM,
            accumulate,
            tuple(jnp.zeros((COMP, CELLS), jnp.float32) for _ in NEAR),
            unroll=8,
        )
        gains = [g * taper(dx, dy) for g, (dx, dy) in zip(gains, NEAR)]

        def updated(m):
            block = fields[m]
            for d, gain in enumerate(gains):
                block = block - scaled[d, pl.ds(m, 1), :] * gain
            return block

        def apply(m, carry):
            if batch + 1 < NB:
                fields[m] = updated(m)
            else:
                anom_out[m] = updated(m)
            return carry

        lax.fori_loop(0, MEM, apply, 0, unroll=8)
        if batch + 1 < NB:
            fields[MEM] = updated(MEM)
        else:
            mean_out[...] = updated(MEM)


def local(
    atm_members,
    ocean_members,
    remap_weights,
    pair_src,
    obs_cell,
    obs_value,
    obs_error,
    obs_live,
    obs_order,
):
    f32 = jnp.float32
    vmem = pl.BlockSpec(memory_space=pltpu.VMEM)
    anywhere = pl.BlockSpec(memory_space=pl.ANY)
    dma = pltpu.SemaphoreType.DMA
    state, meta = pl.pallas_call(
        exchange_kernel,
        out_shape=(
            jax.ShapeDtypeStruct((4, ROWS, CELLS), f32),
            jax.ShapeDtypeStruct((OBS, CELLS), f32),
        ),
        in_specs=[pl.BlockSpec(memory_space=pltpu.SMEM), anywhere, anywhere] + [vmem] * 5,
        out_specs=(vmem, vmem),
        scratch_shapes=[
            pltpu.VMEM((9, CHUNKS, MEM, CW), jnp.bfloat16),
            pltpu.VMEM((K, OCN_DEV, CELLS), jnp.bfloat16),
            pltpu.VMEM((MEM, CELLS), f32),
            pltpu.VMEM((8, CELLS), f32),
            pltpu.VMEM((9, 8, CELLS), f32),
            pltpu.VMEM((2, 16, CELLS), f32),
            pltpu.VMEM((2, 24, CELLS), f32),
            pltpu.VMEM((3, 16, CELLS), f32),
            pltpu.VMEM((3, 16, CELLS), f32),
            pltpu.VMEM((24, CELLS), f32),
            pltpu.VMEM((24, CELLS), f32),
            dma((CHUNKS + 1,)),
            dma((9, CHUNKS)),
            dma((9, CHUNKS)),
            dma((9, CHUNKS)),
            dma((9,)),
            dma((9,)),
            dma((9,)),
            dma((9,)),
        ],
        compiler_params=pltpu.CompilerParams(
            collective_id=0, has_side_effects=True, vmem_limit_bytes=16 * 1024 * 1024
        ),
    )(
        pair_src[0],
        ocean_members[0, 0],
        remap_weights[0, 0],
        obs_cell[0],
        obs_value[0],
        obs_error[0],
        obs_live[0],
        obs_order[0],
    )
    mean, anomaly = pl.pallas_call(
        update_kernel,
        out_shape=(
            jax.ShapeDtypeStruct((COMP, CELLS), f32),
            jax.ShapeDtypeStruct((MEM, COMP, CELLS), f32),
        ),
        in_specs=[vmem] * 3,
        out_specs=(vmem, vmem),
        scratch_shapes=[
            pltpu.VMEM((4, ROWS, CELLS), f32),
            pltpu.VMEM((MEM + 1, COMP, CELLS), f32),
            pltpu.VMEM((4, 9, MEM, CELLS), f32),
            pltpu.VMEM((9, ROWS, CELLS), f32),
            pltpu.VMEM((8, CELLS), f32),
        ],
        compiler_params=pltpu.CompilerParams(vmem_limit_bytes=16 * 1024 * 1024),
    )(state, meta, atm_members[0, 0])
    return (mean[None, None], anomaly[None, None])


def solution(mesh):
    in_specs = (
        P("gx", "gy", None, None, None),
        P("gx", "gy", None, None),
        P("gx", "gy", None, None, None),
        P("gx", "gy", None),
        P("gx", "gy", None),
        P("gx", "gy", None),
        P("gx", "gy", None),
        P("gx", "gy", None),
        P("gx", "gy", None),
    )
    out_specs = (P("gx", "gy", None, None), P("gx", "gy", None, None, None))
    return jax.shard_map(local, mesh=mesh, in_specs=in_specs, out_specs=out_specs, check_vma=False)
```

```python
import functools

import jax
import jax.numpy as jnp
from jax import lax
from jax.experimental import pallas as pl
from jax.experimental.pallas import tpu as pltpu
from jax.sharding import PartitionSpec as P

MEM = 80
AX = 8
AY = 16
OCN_DEV = 1024
OB = 32
NB = 2
K = 4
FIELDS = 12
COMP = 13
CELLS = 128
OBS = 64
ROWS = 88
GROUPS = 11
CHUNKS = 4
CW = OCN_DEV // CHUNKS
DIRECT = 3

MESH = pl.DeviceIdType.MESH
NEAR = [(dx, dy) for dx in (-1, 0, 1) for dy in (-1, 0, 1)]
AROUND = [d for d in NEAR if d != (0, 0)]


def slot(dx, dy):
    return (dx + 1) * 3 + dy + 1


def roll(x, shift):
    shift = shift % CELLS
    return x if shift == 0 else pltpu.roll(x, shift, 1)


def exchange_kernel(
    src_hbm,
    ocean,
    weights,
    cell_hbm,
    value_hbm,
    error_hbm,
    live_hbm,
    order_hbm,
    f_out,
    obs_out,
    src,
    ints,
    floats,
    oce,
    wv,
    acc,
    columns,
    meta,
    meta_in,
    pack_y,
    pack_x,
    in_w,
    in_e,
    in_n,
    in_s,
    local_sem,
    oce_send,
    oce_recv,
    relay_send,
    meta_send,
    meta_recv,
    halo_send,
    halo_recv,
):
    i = lax.axis_index("gx")
    j = lax.axis_index("gy")
    nx = lax.axis_size("gx")
    ny = lax.axis_size("gy")

    away = 2 * (i % 2) - 1
    mate = -away
    has_away = jnp.logical_and(i + away >= 0, i + away < nx)
    near = 1 - 2 * ((j % 4 + 3) // 4)
    far = -near
    has_far = jnp.logical_and(j + far >= 0, j + far < ny)
    when_away, when_far = pl.when(has_away), pl.when(has_far)

    def has(dx, dy):
        cond = None
        for pos, step, count in ((i, dx, nx), (j, dy, ny)):
            if step:
                ok = (pos > 0) if step < 0 else (pos < count - 1)
                cond = ok if cond is None else jnp.logical_and(cond, ok)
        return cond

    def when(dx, dy):
        return pl.when(has(dx, dy))

    def device(dx, dy):
        return (i + dx, j + dy)

    barrier = pltpu.get_barrier_semaphore()

    def greet(dx, dy):
        pl.semaphore_signal(barrier, inc=1, device_id=device(dx, dy), device_id_type=MESH)

    @when_far
    def _():
        greet(0, far)

    greet(0, near)

    @when_away
    def _():
        greet(away, 0)

    greet(mate, 0)

    own_load = [
        pltpu.make_async_copy(
            ocean.at[:, pl.ds(c * CW, CW)], oce.at[4, c], local_sem.at[c]
        )
        for c in range(CHUNKS)
    ]
    for copy in own_load:
        copy.start()
    small_load = [
        pltpu.make_async_copy(source, target, local_sem.at[CHUNKS + 1 + n])
        for n, (source, target) in enumerate(
            (
                (cell_hbm, ints.at[0]),
                (live_hbm, ints.at[1]),
                (order_hbm, ints.at[2]),
                (value_hbm, floats.at[0]),
                (error_hbm, floats.at[1]),
                (src_hbm, src),
            )
        )
    ]
    for copy in small_load:
        copy.start()
    w_load = pltpu.make_async_copy(weights, wv, local_sem.at[CHUNKS])
    w_load.start()

    pl.semaphore_wait(
        barrier,
        2 + has_away.astype(jnp.int32) + has_far.astype(jnp.int32),
    )

    def ocean_copy(c, dx, dy, sem):
        return pltpu.make_async_remote_copy(
            src_ref=oce.at[4, c],
            dst_ref=oce.at[slot(-dx, -dy), c],
            send_sem=oce_send.at[sem, c],
            recv_sem=oce_recv.at[slot(-dx, -dy), c],
            device_id=device(dx, dy),
            device_id_type=MESH,
        )

    def relay_copy(c, dx, dy, sem):
        return pltpu.make_async_remote_copy(
            src_ref=oce.at[slot(0, dy), c],
            dst_ref=oce.at[slot(-dx, dy), c],
            send_sem=relay_send.at[sem, c],
            recv_sem=oce_recv.at[slot(-dx, dy), c],
            device_id=device(dx, 0),
            device_id_type=MESH,
        )

    def arrived(c, dx, dy):
        ocean_copy(c, -dx, -dy, 0).wait_recv()

    def meta_copy(dx, dy):
        return pltpu.make_async_remote_copy(
            src_ref=meta,
            dst_ref=meta_in.at[slot(-dx, -dy)],
            send_sem=meta_send.at[slot(dx, dy)],
            recv_sem=meta_recv.at[slot(-dx, -dy)],
            device_id=device(dx, dy),
            device_id_type=MESH,
        )

    for c in range(CHUNKS):
        own_load[c].wait()

        @when_far
        def _():
            ocean_copy(c, 0, far, 1).start()

        ocean_copy(c, 0, near, 0).start()

        @when_away
        def _():
            ocean_copy(c, away, 0, 3).start()

        ocean_copy(c, mate, 0, 2).start()

    for copy in small_load:
        copy.wait()
    lane = lax.broadcasted_iota(jnp.int32, (OBS, OBS), 0)
    perm = jnp.where(lane == ints[2], 1.0, 0.0)
    rows = [
        ints[0].astype(jnp.float32),
        floats[0],
        floats[1],
        ints[1].astype(jnp.float32),
    ]
    stacked = jnp.concatenate(rows + [jnp.zeros((4, OBS), jnp.float32)], axis=0)
    ordered = jnp.dot(
        stacked,
        perm,
        precision=lax.Precision.HIGHEST,
        preferred_element_type=jnp.float32,
    )
    meta[...] = jnp.concatenate([ordered, jnp.zeros((8, CELLS - OBS), jnp.float32)], axis=1)

    positions = [
        (src[0, k] // ny - i + 1) * 3 + (src[0, k] % ny - j + 1) for k in range(K)
    ]

    def product(dx, dy, c):
        p = slot(dx, dy)
        which = jnp.int32(0)
        valid = positions[0] == p
        for k in range(1, K):
            which = jnp.where(positions[k] == p, k, which)
            valid = jnp.logical_or(valid, positions[k] == p)
        part = jnp.dot(
            oce[p, c],
            wv[which, pl.ds(c * CW, CW), :],
            preferred_element_type=jnp.float32,
        )
        return jnp.where(valid, part, 0.0)

    w_load.wait()
    total = product(0, 0, 0)
    for c in range(1, CHUNKS):
        total = total + product(0, 0, c)
    acc[...] = total

    def pass_on(c, dy, index):
        relay_copy(c, mate, dy, 2 * index).start()

        @when_away
        def _():
            if c < DIRECT:
                relay_copy(c, away, dy, 2 * index + 1).start()
            if c == 0:
                for direct in range(DIRECT, CHUNKS):
                    ocean_copy(direct, away, dy, 4 + index).start()

    for step in range(CHUNKS + 1):
        if step < CHUNKS:
            arrived(step, 0, near)
            pass_on(step, near, 0)
        if step > 0:

            @when_far
            def _():
                arrived(step - 1, 0, far)
                pass_on(step - 1, far, 1)

        if step == 1:
            for dx, dy in AROUND:

                @when(dx, dy)
                def _():
                    meta_copy(dx, dy).start()

        if step < CHUNKS:
            arrived(step, mate, 0)
            acc[...] += product(mate, 0, step) + product(0, near, step)

            @when_away
            def _():
                arrived(step, away, 0)
                acc[...] += product(away, 0, step)

        if step > 0:

            @when_far
            def _():
                acc[...] += product(0, far, step - 1)

    for c in range(CHUNKS):
        arrived(c, mate, near)
        acc[...] += product(mate, near, c)

        @when_far
        def _():
            arrived(c, mate, far)
            acc[...] += product(mate, far, c)

    for c in range(CHUNKS):

        @when_away
        def _():
            arrived(c, away, near)
            acc[...] += product(away, near, c)

            @when_far
            def _():
                arrived(c, away, far)
                acc[...] += product(away, far, c)

    sst = acc[...]
    mean = jnp.sum(sst, axis=0, keepdims=True) / MEM
    anomaly = sst - mean
    pieces = [anomaly[8 * g : 8 * g + 8] for g in range(MEM // 8)]
    pieces.append(jnp.broadcast_to(mean, (8, CELLS)))
    lane8 = lax.broadcasted_iota(jnp.int32, (8, CELLS), 1)
    pair = (lane8 % AY) // 2
    quarter = lane8 // 32

    for block in range(2):
        west = jnp.zeros((8, CELLS), jnp.float32)
        east = west
        for g in range(8 * block, min(8 * block + 8, GROUPS)):
            s = g % 8
            west = jnp.where(pair == s, roll(pieces[g], 2 * s), west)
            east = jnp.where(pair == 7 - s, roll(pieces[g], -2 * s), east)
        pack_y[0, 8 * block : 8 * block + 8, :] = west
        pack_y[1, 8 * block : 8 * block + 8, :] = east
    for block in range(3):
        north = jnp.zeros((8, CELLS), jnp.float32)
        south = north
        for g in range(4 * block, min(4 * block + 4, GROUPS)):
            s = g % 4
            north = jnp.where(quarter == s, roll(pieces[g], 32 * s), north)
            south = jnp.where(quarter == 3 - s, roll(pieces[g], -32 * s), south)
        pack_x[0, 8 * block : 8 * block + 8, :] = north
        pack_x[1, 8 * block : 8 * block + 8, :] = south

    def halo_copy(dx, dy):
        if dy < 0:
            source, target = pack_y.at[0], in_w.at[1 - dx]
        elif dy > 0:
            source, target = pack_y.at[1], in_e.at[1 - dx]
        elif dx < 0:
            source, target = pack_x.at[0], in_n
        else:
            source, target = pack_x.at[1], in_s
        return pltpu.make_async_remote_copy(
            src_ref=source,
            dst_ref=target,
            send_sem=halo_send.at[slot(dx, dy)],
            recv_sem=halo_recv.at[slot(-dx, -dy)],
            device_id=device(dx, dy),
            device_id_type=MESH,
        )

    f_out[0, :MEM, :] = anomaly
    f_out[0, MEM:, :] = pieces[-1]

    for dx, dy in ((1, 1), (1, -1), (-1, 1), (-1, -1), (0, 1), (0, -1), (1, 0), (-1, 0)):

        @when(dx, dy)
        def _():
            halo_copy(dx, dy).start()

    absent = jnp.where(lax.broadcasted_iota(jnp.int32, (8, CELLS), 0) == 2, 1.0, 0.0)
    for dx, dy in AROUND:

        @when(dx, dy)
        def _():
            meta_copy(-dx, -dy).wait_recv()

    blocks = []
    for dx, dy in NEAR:
        if (dx, dy) == (0, 0):
            blocks.append(meta[...])
        else:
            blocks.append(jnp.where(has(dx, dy), meta_in[slot(dx, dy)], absent))
    blocks.append(jnp.zeros((CELLS - 72, CELLS), jnp.float32))
    columns[...] = jnp.concatenate(blocks, axis=0).T

    lane32 = lax.broadcasted_iota(jnp.int32, (OB, CELLS), 1)
    lanes = lane32.astype(jnp.float32)
    low_x32, low_y32 = lane32 < 64, (lane32 % AY) < 8
    for batch in range(NB):
        rows = slice(batch * OB, (batch + 1) * OB)

        def dense(dx, dy):
            at = 8 * slot(dx, dy)
            cells, values, errors, alive = (
                jnp.broadcast_to(columns[rows, at + n : at + n + 1], (OB, CELLS))
                for n in range(4)
            )
            hit = jnp.where(cells == lanes, alive, 0.0)
            return hit, hit * values, errors + (1.0 - alive), errors

        def either(mask, first, second):
            return tuple(jnp.where(mask, a, b) for a, b in zip(first, second))

        places = [
            lambda: dense(0, 0),
            lambda: either(low_x32, dense(1, 0), dense(-1, 0)),
            lambda: either(low_y32, dense(0, 1), dense(0, -1)),
            lambda: either(
                low_y32,
                either(low_x32, dense(1, 1), dense(-1, 1)),
                either(low_x32, dense(1, -1), dense(-1, -1)),
            ),
        ]
        for f, place in enumerate(places):
            for n, part in enumerate(place()):
                obs_out[batch, f, n] = part

    for c in range(CHUNKS):
        ocean_copy(c, 0, near, 0).wait_send()
        ocean_copy(c, mate, 0, 2).wait_send()
        relay_copy(c, mate, near, 0).wait_send()

        @when_far
        def _():
            ocean_copy(c, 0, far, 1).wait_send()
            relay_copy(c, mate, far, 2).wait_send()

        @when_away
        def _():
            ocean_copy(c, away, 0, 3).wait_send()
            for dy, index, there in ((near, 0, None), (far, 1, has_far)):

                def finish():
                    if c < DIRECT:
                        relay_copy(c, away, dy, 2 * index + 1).wait_send()
                    else:
                        ocean_copy(c, away, dy, 4 + index).wait_send()

                finish() if there is None else pl.when(there)(finish)

    for dx, dy in AROUND:

        @when(dx, dy)
        def _():
            meta_copy(dx, dy).wait_send()

    for dx, dy in AROUND:

        @when(dx, dy)
        def _():
            halo_copy(-dx, -dy).wait_recv()

    low_y = (lane8 % AY) < 8
    low_x = lane8 < 64
    zero = jnp.zeros((8, CELLS), jnp.float32)

    def present(ref, dx, dy):
        return jnp.where(has(dx, dy), ref[...], 0.0)

    north = present(in_n, 1, 0)
    south = present(in_s, -1, 0)
    west = present(in_w.at[1], 0, 1)
    east = present(in_e.at[1], 0, -1)
    low16 = lax.broadcasted_iota(jnp.int32, (16, CELLS), 1) < 64
    west_c = jnp.where(low16, present(in_w.at[2], 1, 1), present(in_w.at[0], -1, 1))
    east_c = jnp.where(low16, present(in_e.at[2], 1, -1), present(in_e.at[0], -1, -1))
    for g in range(GROUPS):
        at = pl.ds(8 * g, 8)
        b, s = g // 4, g % 4
        f_out[1, at, :] = jnp.where(
            low_x,
            roll(north[8 * b : 8 * b + 8], -32 * s),
            roll(south[8 * b : 8 * b + 8], 32 * s),
        )
        b, s = g // 8, g % 8
        for place, w, e in ((2, west, east), (3, west_c, east_c)):
            f_out[place, at, :] = jnp.where(
                low_y,
                roll(w[8 * b : 8 * b + 8], -2 * s),
                roll(e[8 * b : 8 * b + 8], 2 * s),
            )

    for dx, dy in AROUND:

        @when(dx, dy)
        def _():
            halo_copy(dx, dy).wait_send()


def update_kernel(
    f_in,
    obs,
    atm,
    mean_out,
    anom_out,
    state,
    shifted,
    factors,
    result,
    means,
    out_sem,
    mean_sem,
):
    lane8 = lax.broadcasted_iota(jnp.int32, (8, CELLS), 1)
    y8 = lane8 % AY
    first_y, last_y = y8 == 0, y8 == AY - 1
    first_x, last_x = lane8 < AY, lane8 >= CELLS - AY
    groups = range(MEM // 8)

    def at(g):
        return slice(8 * g, 8 * g + 8)

    def shift_all(blocks, wanted):
        out = {}
        turned = {}
        for f in range(4):
            if any((f ^ a) in wanted for a in (0, 1)):
                other = blocks[f ^ 2]
                turned[f, 0] = blocks[f]
                turned[f, 1] = jnp.where(last_y, roll(other, 15), roll(blocks[f], -1))
                turned[f, -1] = jnp.where(first_y, roll(other, -15), roll(blocks[f], 1))
        for f in wanted:
            for dy in (-1, 0, 1):
                own, other = turned[f, dy], turned[f ^ 1, dy]
                out[f, slot(0, dy)] = own
                out[f, slot(1, dy)] = roll(jnp.where(first_x, other, own), -AY)
                out[f, slot(-1, dy)] = roll(jnp.where(last_x, other, own), AY)
        return out

    def allsum(x):
        for step in (4, 2, 1):
            x = x + pltpu.roll(x, step, 0)
        return x

    zero = jnp.zeros((8, CELLS), jnp.float32)
    tapers = [
        max(1.0 - (dx * dx + dy * dy) / 4.0, 0.0) ** 2 / (MEM - 1) for dx, dy in NEAR
    ]

    for batch in range(NB):
        source = f_in if batch == 0 else state
        wanted = (0, 1, 2, 3) if batch == 0 else (0,)
        base = 0 if batch == 0 else 36

        alphas, betas = [], []
        for f in range(4):
            square = zero
            for g in groups:
                block = source[f, at(g), :]
                square = square + block * block
            variance = allsum(square) / (MEM - 1)
            total = [zero, zero, zero]
            for q in range(OB // 8):
                masked = obs[batch, f, 0, at(q), :]
                masked_value = obs[batch, f, 1, at(q), :]
                inverse = 1.0 / (variance + obs[batch, f, 2, at(q), :])
                ratio = obs[batch, f, 3, at(q), :] * inverse
                damping = 1.0 / (1.0 + ratio * lax.rsqrt(ratio))
                weighting = masked * inverse
                total[0] = total[0] + weighting * damping
                total[1] = total[1] + weighting
                total[2] = total[2] + masked_value * inverse
            betas.append(allsum(total[0]))
            alphas.append(allsum(total[2]) - source[f, MEM:, :] * allsum(total[1]))
        alphas = shift_all(alphas, wanted)
        betas = shift_all(betas, wanted)
        alphas = {key: alphas[key] * tapers[key[1]] for key in alphas}
        betas = {key: betas[key] * tapers[key[1]] for key in betas}
        for d in range(9):
            factors[batch, 0, d] = alphas[0, d]
            factors[batch, 1, d] = betas[0, d]

        for g in groups:
            moved = shift_all([source[f, at(g), :] for f in range(4)], wanted)
            for f in wanted:
                for d in range(9):
                    shifted[base + 9 * f + d, at(g), :] = moved[f, d]

        for f in wanted:
            sums = [zero] * 9
            for g in groups:
                block = source[f, at(g), :]
                for d in range(9):
                    sums[d] = sums[d] + shifted[base + 9 * f + d, at(g), :] * block
            sums = [allsum(x) for x in sums]
            mean = source[f, MEM:, :]
            for d in range(9):
                mean = mean + alphas[f, d] * sums[d]
            gains = [betas[f, d] * sums[d] for d in range(9)]
            for g in groups:
                block = source[f, at(g), :]
                for d in range(9):
                    block = block - shifted[base + 9 * f + d, at(g), :] * gains[d]
                if batch + 1 < NB:
                    state[f, at(g), :] = block
                else:
                    result[FIELDS, at(g), :] = block
            if batch + 1 < NB:
                state[f, MEM:, :] = mean
            else:
                means[FIELDS] = mean[:1]

    def sst_copy():
        return pltpu.make_async_copy(result.at[FIELDS], anom_out.at[FIELDS], mean_sem.at[1])

    def field_copy(pair):
        part = pl.ds(2 * pair, 2)
        return pltpu.make_async_copy(result.at[part], anom_out.at[part], out_sem.at[pair])

    sst_copy().start()

    def two_fields(pair, carry):
        fields = (2 * pair, 2 * pair + 1)
        sums = [zero, zero]
        for g in groups:
            for u in range(2):
                sums[u] = sums[u] + atm[fields[u], at(g), :]
        mean = [allsum(x) / MEM for x in sums]
        for batch in range(NB):
            sums = [[zero] * 9, [zero] * 9]
            for g in groups:
                for u in range(2):
                    if batch == 0:
                        block = atm[fields[u], at(g), :] - mean[u]
                        result[fields[u], at(g), :] = block
                    else:
                        block = result[fields[u], at(g), :]
                    for d in range(9):
                        sums[u][d] = sums[u][d] + shifted[36 * batch + d, at(g), :] * block
            sums = [[allsum(x) for x in sums[u]] for u in range(2)]
            for u in range(2):
                for d in range(9):
                    mean[u] = mean[u] + factors[batch, 0, d] * sums[u][d]
            gains = [[factors[batch, 1, d] * sums[u][d] for d in range(9)] for u in range(2)]
            for g in groups:
                for u in range(2):
                    block = result[fields[u], at(g), :]
                    for d in range(9):
                        block = block - shifted[36 * batch + d, at(g), :] * gains[u][d]
                    result[fields[u], at(g), :] = block
        for u in range(2):
            means[fields[u]] = mean[u][:1]
        field_copy(pair).start()
        return carry

    lax.fori_loop(0, FIELDS // 2, two_fields, 0)
    mean_copy = pltpu.make_async_copy(means, mean_out, mean_sem.at[0])
    mean_copy.start()
    sst_copy().wait()
    for pair in range(FIELDS // 2):
        field_copy(pair).wait()
    mean_copy.wait()


def local(
    atm_members,
    ocean_members,
    remap_weights,
    pair_src,
    obs_cell,
    obs_value,
    obs_error,
    obs_live,
    obs_order,
):
    f32 = jnp.float32
    vmem = pl.BlockSpec(memory_space=pltpu.VMEM)
    hbm = pl.BlockSpec(memory_space=pltpu.HBM)
    dma = pltpu.SemaphoreType.DMA
    state, meta = pl.pallas_call(
        exchange_kernel,
        out_shape=(
            jax.ShapeDtypeStruct((4, ROWS, CELLS), f32),
            jax.ShapeDtypeStruct((NB, 4, 4, OB, CELLS), f32),
        ),
        in_specs=[hbm] * 8,
        out_specs=(vmem, vmem),
        scratch_shapes=[
            pltpu.SMEM((1, K), jnp.int32),
            pltpu.VMEM((3, 1, OBS), jnp.int32),
            pltpu.VMEM((2, 1, OBS), f32),
            pltpu.VMEM((9, CHUNKS, MEM, CW), jnp.bfloat16),
            pltpu.VMEM((K, OCN_DEV, CELLS), jnp.bfloat16),
            pltpu.VMEM((MEM, CELLS), f32),
            pltpu.VMEM((CELLS, CELLS), f32),
            pltpu.VMEM((8, CELLS), f32),
            pltpu.VMEM((9, 8, CELLS), f32),
            pltpu.VMEM((2, 16, CELLS), f32),
            pltpu.VMEM((2, 24, CELLS), f32),
            pltpu.VMEM((3, 16, CELLS), f32),
            pltpu.VMEM((3, 16, CELLS), f32),
            pltpu.VMEM((24, CELLS), f32),
            pltpu.VMEM((24, CELLS), f32),
            dma((CHUNKS + 7,)),
            dma((9, CHUNKS)),
            dma((9, CHUNKS)),
            dma((9, CHUNKS)),
            dma((9,)),
            dma((9,)),
            dma((9,)),
            dma((9,)),
        ],
        compiler_params=pltpu.CompilerParams(
            collective_id=0, has_side_effects=True, vmem_limit_bytes=16 * 1024 * 1024
        ),
    )(
        *(
            pltpu.with_memory_space_constraint(x, pltpu.HBM)
            for x in (
                pair_src[0],
                ocean_members[0, 0],
                remap_weights[0, 0],
                obs_cell[0],
                obs_value[0],
                obs_error[0],
                obs_live[0],
                obs_order[0],
            )
        )
    )
    mean, anomaly = pl.pallas_call(
        update_kernel,
        out_shape=(
            jax.ShapeDtypeStruct((COMP, 1, CELLS), f32),
            jax.ShapeDtypeStruct((COMP, MEM, CELLS), f32),
        ),
        in_specs=[vmem] * 3,
        out_specs=(hbm, hbm),
        scratch_shapes=[
            pltpu.VMEM((4, ROWS, CELLS), f32),
            pltpu.VMEM((45, MEM, CELLS), f32),
            pltpu.VMEM((NB, 2, 9, 8, CELLS), f32),
            pltpu.VMEM((COMP, MEM, CELLS), f32),
            pltpu.VMEM((COMP, 1, CELLS), f32),
            dma((FIELDS // 2,)),
            dma((2,)),
        ],
        compiler_params=pltpu.CompilerParams(vmem_limit_bytes=16 * 1024 * 1024),
    )(state, meta, jnp.transpose(atm_members[0, 0], (1, 0, 2)))
    return (mean.reshape(1, 1, COMP, CELLS), jnp.transpose(anomaly, (1, 0, 2))[None, None])


def solution(mesh):
    in_specs = (
        P("gx", "gy", None, None, None),
        P("gx", "gy", None, None),
        P("gx", "gy", None, None, None),
        P("gx", "gy", None),
        P("gx", "gy", None),
        P("gx", "gy", None),
        P("gx", "gy", None),
        P("gx", "gy", None),
        P("gx", "gy", None),
    )
    out_specs = (P("gx", "gy", None, None), P("gx", "gy", None, None, None))
    return jax.shard_map(local, mesh=mesh, in_specs=in_specs, out_specs=out_specs, check_vma=False)
```

```python
import functools

import jax
import jax.numpy as jnp
from jax import lax
from jax.experimental import pallas as pl
from jax.experimental.pallas import tpu as pltpu
from jax.sharding import PartitionSpec as P

MEM = 80
AX = 8
AY = 16
OCN_DEV = 1024
OB = 32
NB = 2
K = 4
FIELDS = 12
COMP = 13
CELLS = 128
OBS = 64
ROWS = 88
GROUPS = 11
CHUNKS = 4
CW = OCN_DEV // CHUNKS
FIRST, SECOND, THIRD, BOTH, WHOLE = (0, 1), (1, 1), (2, 2), (0, 2), (0, 4)

MESH = pl.DeviceIdType.MESH
NEAR = [(dx, dy) for dx in (-1, 0, 1) for dy in (-1, 0, 1)]
AROUND = [d for d in NEAR if d != (0, 0)]


def slot(dx, dy):
    return (dx + 1) * 3 + dy + 1


def roll(x, shift):
    shift = shift % CELLS
    return x if shift == 0 else pltpu.roll(x, shift, 1)


def exchange_kernel(
    src_hbm,
    ocean,
    weights,
    cell_hbm,
    value_hbm,
    error_hbm,
    live_hbm,
    order_hbm,
    f_out,
    obs_out,
    src,
    ints,
    floats,
    oce,
    wv,
    acc,
    columns,
    meta_in,
    pack_y,
    pack_x,
    in_y,
    in_x,
    local_sem,
    oce_send,
    oce_recv,
    meta_send,
    meta_recv,
    halo_send,
    halo_recv,
):
    i = lax.axis_index("gx")
    j = lax.axis_index("gy")
    nx = lax.axis_size("gx")
    ny = lax.axis_size("gy")

    away = 2 * (i % 2) - 1
    mate = -away
    has_away = jnp.logical_and(i + away >= 0, i + away < nx)
    near = 1 - 2 * ((j % 4 + 3) // 4)
    far = -near
    has_far = jnp.logical_and(j + far >= 0, j + far < ny)
    when_away, when_far = pl.when(has_away), pl.when(has_far)

    def has(dx, dy):
        cond = None
        for pos, step, count in ((i, dx, nx), (j, dy, ny)):
            if step:
                ok = (pos > 0) if step < 0 else (pos < count - 1)
                cond = ok if cond is None else jnp.logical_and(cond, ok)
        return cond

    def when(dx, dy):
        return pl.when(has(dx, dy))

    def device(dx, dy):
        return (i + dx, j + dy)

    own_load = [
        pltpu.make_async_copy(
            ocean.at[:, pl.ds(c * CW, CW)], oce.at[4, c], local_sem.at[c]
        )
        for c in range(CHUNKS)
    ]
    for copy in own_load:
        copy.start()

    barrier = pltpu.get_barrier_semaphore()

    def greet(dx, dy):
        pl.semaphore_signal(barrier, inc=1, device_id=device(dx, dy), device_id_type=MESH)

    @when_far
    def _():
        greet(0, far)

    greet(0, near)

    @when_away
    def _():
        greet(away, 0)

    greet(mate, 0)

    pl.semaphore_wait(
        barrier,
        2 + has_away.astype(jnp.int32) + has_far.astype(jnp.int32),
    )

    def tile(p, piece):
        return oce.at[p, pl.ds(*piece)]

    def ocean_copy(piece, from_dx, from_dy, dx, dy, sem):
        target = slot(from_dx - dx, from_dy - dy)
        return pltpu.make_async_remote_copy(
            src_ref=tile(slot(from_dx, from_dy), piece),
            dst_ref=tile(target, piece),
            send_sem=oce_send.at[sem],
            recv_sem=oce_recv.at[target, piece[0]],
            device_id=device(dx, dy),
            device_id_type=MESH,
        )

    def arrived(piece, dx, dy):
        ocean_copy(piece, 0, 0, -dx, -dy, 0).wait_recv()

    def meta_copy(dx, dy, sem):
        if isinstance(dx, int):
            source, target = meta_in.at[4], meta_in.at[slot(0, -dy)]
            recv = meta_recv.at[slot(0, -dy)]
        else:
            source, target = meta_in.at[pl.ds(3, 3)], meta_in.at[pl.ds(slot(-dx, -1), 3)]
            recv = meta_recv.at[slot(-dx, 0)]
        return pltpu.make_async_remote_copy(
            src_ref=source,
            dst_ref=target,
            send_sem=meta_send.at[sem],
            recv_sem=recv,
            device_id=device(dx, dy),
            device_id_type=MESH,
        )

    sends = []

    def send(far_needed, away_needed, *spec):
        sends.append((far_needed, away_needed, spec + (len(sends),)))
        ocean_copy(*sends[-1][2]).start()

    for c in range(CHUNKS):
        own_load[c].wait()
        if c == 0:
            send(False, False, FIRST, 0, 0, 0, near)
            when_far(lambda: send(True, False, FIRST, 0, 0, 0, far))
        if c == 1:
            send(False, False, SECOND, 0, 0, 0, near)
            when_far(lambda: send(True, False, SECOND, 0, 0, 0, far))
        if c == 3:

            @when_away
            def _():
                send(False, True, THIRD, 0, 0, away, 0)
                send(False, True, BOTH, 0, 0, away, 0)

            send(False, False, THIRD, 0, 0, 0, near)
            when_far(lambda: send(True, False, THIRD, 0, 0, 0, far))
            send(False, False, WHOLE, 0, 0, mate, 0)

    small_load = [
        pltpu.make_async_copy(source, target, local_sem.at[CHUNKS + 1 + n])
        for n, (source, target) in enumerate(
            (
                (cell_hbm, ints.at[0]),
                (live_hbm, ints.at[1]),
                (order_hbm, ints.at[2]),
                (value_hbm, floats.at[0]),
                (error_hbm, floats.at[1]),
                (src_hbm, src),
            )
        )
    ]
    for copy in small_load:
        copy.start()
    w_load = pltpu.make_async_copy(weights, wv, local_sem.at[CHUNKS])
    w_load.start()

    for copy in small_load:
        copy.wait()
    lane = lax.broadcasted_iota(jnp.int32, (OBS, OBS), 0)
    perm = jnp.where(lane == ints[2], 1.0, 0.0)
    rows = [
        ints[0].astype(jnp.float32),
        floats[0],
        floats[1],
        ints[1].astype(jnp.float32),
    ]
    stacked = jnp.concatenate(rows + [jnp.zeros((4, OBS), jnp.float32)], axis=0)
    ordered = jnp.dot(
        stacked,
        perm,
        precision=lax.Precision.HIGHEST,
        preferred_element_type=jnp.float32,
    )
    meta_in[4] = jnp.concatenate([ordered, jnp.zeros((8, CELLS - OBS), jnp.float32)], axis=1)

    @pl.when(jnp.logical_not(has_far))
    def _():
        meta_in[slot(0, far)] = jnp.zeros((8, CELLS), jnp.float32)


    positions = [
        (src[0, k] // ny - i + 1) * 3 + (src[0, k] % ny - j + 1) for k in range(K)
    ]

    def product(dx, dy, c):
        p = slot(dx, dy)
        which = jnp.int32(0)
        valid = positions[0] == p
        for k in range(1, K):
            which = jnp.where(positions[k] == p, k, which)
            valid = jnp.logical_or(valid, positions[k] == p)
        part = jnp.dot(
            oce[p, c],
            wv[which, pl.ds(c * CW, CW), :],
            preferred_element_type=jnp.float32,
        )
        return jnp.where(valid, part, 0.0)

    w_load.wait()
    total = product(0, 0, 0)
    for c in range(1, CHUNKS):
        total = total + product(0, 0, c)
    acc[...] = total

    def add(dx, dy, piece):
        for c in range(piece[0], piece[0] + piece[1]):
            acc[...] += product(dx, dy, c)

    def from_y(piece, with_away):
        def one(dy, is_far):
            arrived(piece, 0, dy)
            send(is_far, False, piece, 0, dy, mate, 0)
            if with_away:
                when_away(lambda: send(is_far, True, piece, 0, dy, away, 0))

        one(near, False)
        when_far(lambda: one(far, True))

    from_y(FIRST, True)
    meta_copy(0, near, 0).start()
    when_far(lambda: meta_copy(0, far, 1).start())

    @when_away
    def _():
        arrived(THIRD, away, 0)
        send(False, True, THIRD, away, 0, 0, near)
        when_far(lambda: send(True, True, THIRD, away, 0, 0, far))

    from_y(SECOND, True)
    arrived(WHOLE, mate, 0)
    add(mate, 0, WHOLE)
    add(0, near, BOTH)
    when_far(lambda: add(0, far, BOTH))
    when_away(lambda: add(away, 0, THIRD))
    from_y(THIRD, False)
    add(0, near, THIRD)
    when_far(lambda: add(0, far, THIRD))

    meta_copy(0, -near, 0).wait_recv()
    when_far(lambda: meta_copy(0, -far, 1).wait_recv())
    meta_copy(mate, 0, 2).start()
    when_away(lambda: meta_copy(away, 0, 3).start())

    @when_away
    def _():
        arrived(BOTH, away, 0)
        add(away, 0, BOTH)

    def corner(dx, dy, piece):
        arrived(piece, dx, dy)
        add(dx, dy, piece)

    for piece in (FIRST, SECOND, THIRD):
        corner(mate, near, piece)
        when_far(lambda: corner(mate, far, piece))

    for piece in (FIRST, SECOND, THIRD):

        @when_away
        def _():
            corner(away, near, piece)
            when_far(lambda: corner(away, far, piece))

    sst = acc[...]
    mean = jnp.sum(sst, axis=0, keepdims=True) / MEM
    anomaly = sst - mean
    pieces = [anomaly[8 * g : 8 * g + 8] for g in range(MEM // 8)]
    pieces.append(jnp.broadcast_to(mean, (8, CELLS)))
    lane8 = lax.broadcasted_iota(jnp.int32, (8, CELLS), 1)
    pair = (lane8 % AY) // 2
    quarter = lane8 // 32

    for block in range(2):
        west = jnp.zeros((8, CELLS), jnp.float32)
        east = west
        for g in range(8 * block, min(8 * block + 8, GROUPS)):
            s = g % 8
            west = jnp.where(pair == s, roll(pieces[g], 2 * s), west)
            east = jnp.where(pair == 7 - s, roll(pieces[g], -2 * s), east)
        pack_y[0, 8 * block : 8 * block + 8, :] = west
        pack_y[1, 8 * block : 8 * block + 8, :] = east
    for block in range(3):
        north = jnp.zeros((8, CELLS), jnp.float32)
        south = north
        for g in range(4 * block, min(4 * block + 4, GROUPS)):
            s = g % 4
            north = jnp.where(quarter == s, roll(pieces[g], 32 * s), north)
            south = jnp.where(quarter == 3 - s, roll(pieces[g], -32 * s), south)
        pack_x[0, 8 * block : 8 * block + 8, :] = north
        pack_x[1, 8 * block : 8 * block + 8, :] = south

    def halo_y(dx, dy):
        side = (dy + 1) // 2
        return pltpu.make_async_remote_copy(
            src_ref=pack_y.at[side],
            dst_ref=in_y.at[side, 1 - dx],
            send_sem=halo_send.at[slot(dx, dy)],
            recv_sem=halo_recv.at[slot(-dx, -dy)],
            device_id=device(dx, dy),
            device_id_type=MESH,
        )

    def halo_x(dx):
        side = (dx + 1) // 2
        return pltpu.make_async_remote_copy(
            src_ref=pack_x.at[side],
            dst_ref=in_x.at[side],
            send_sem=halo_send.at[slot(dx, 0)],
            recv_sem=halo_recv.at[slot(-dx, 0)],
            device_id=device(dx, 0),
            device_id_type=MESH,
        )

    @when_away
    def _():
        when_far(lambda: halo_y(away, far).start())
        halo_y(away, near).start()

    @when_far
    def _():
        halo_y(mate, far).start()
        halo_y(0, far).start()

    halo_y(mate, near).start()
    halo_y(0, near).start()
    when_away(lambda: halo_x(away).start())
    halo_x(mate).start()

    f_out[0, :MEM, :] = anomaly
    f_out[0, MEM:, :] = pieces[-1]

    absent = jnp.where(lax.broadcasted_iota(jnp.int32, (8, CELLS), 0) == 2, 1.0, 0.0)
    meta_copy(-mate, 0, 2).wait_recv()
    when_away(lambda: meta_copy(-away, 0, 3).wait_recv())

    blocks = []
    for dx, dy in NEAR:
        if (dx, dy) == (0, 0):
            blocks.append(meta_in[4])
        else:
            blocks.append(jnp.where(has(dx, dy), meta_in[slot(dx, dy)], absent))
    blocks.append(jnp.zeros((CELLS - 72, CELLS), jnp.float32))
    columns[...] = jnp.concatenate(blocks, axis=0).T

    lane32 = lax.broadcasted_iota(jnp.int32, (OB, CELLS), 1)
    lanes = lane32.astype(jnp.float32)
    low_x32, low_y32 = lane32 < 64, (lane32 % AY) < 8
    for batch in range(NB):
        rows = slice(batch * OB, (batch + 1) * OB)

        def dense(dx, dy):
            at = 8 * slot(dx, dy)
            cells, values, errors, alive = (
                jnp.broadcast_to(columns[rows, at + n : at + n + 1], (OB, CELLS))
                for n in range(4)
            )
            hit = jnp.where(cells == lanes, alive, 0.0)
            return hit, hit * values, errors + (1.0 - alive), errors

        def either(mask, first, second):
            return tuple(jnp.where(mask, a, b) for a, b in zip(first, second))

        places = [
            lambda: dense(0, 0),
            lambda: either(low_x32, dense(1, 0), dense(-1, 0)),
            lambda: either(low_y32, dense(0, 1), dense(0, -1)),
            lambda: either(
                low_y32,
                either(low_x32, dense(1, 1), dense(-1, 1)),
                either(low_x32, dense(1, -1), dense(-1, -1)),
            ),
        ]
        for f, place in enumerate(places):
            for n, part in enumerate(place()):
                obs_out[batch, f, n] = part

    def finish(far_needed, away_needed):
        for f, a, spec in sends:
            if (f, a) == (far_needed, away_needed):
                ocean_copy(*spec).wait_send()

    finish(False, False)
    meta_copy(0, near, 0).wait_send()
    meta_copy(mate, 0, 2).wait_send()

    @when_far
    def _():
        finish(True, False)
        meta_copy(0, far, 1).wait_send()

    @when_away
    def _():
        finish(False, True)
        meta_copy(away, 0, 3).wait_send()
        when_far(lambda: finish(True, True))

    halo_x(-mate).wait_recv()
    halo_y(0, -near).wait_recv()
    halo_y(-mate, -near).wait_recv()

    @when_far
    def _():
        halo_y(0, -far).wait_recv()
        halo_y(-mate, -far).wait_recv()

    @when_away
    def _():
        halo_x(-away).wait_recv()
        halo_y(-away, -near).wait_recv()
        when_far(lambda: halo_y(-away, -far).wait_recv())

    low_y = (lane8 % AY) < 8
    low_x = lane8 < 64
    zero = jnp.zeros((8, CELLS), jnp.float32)

    def present(ref, dx, dy):
        return jnp.where(has(dx, dy), ref[...], 0.0)

    north = present(in_x.at[0], 1, 0)
    south = present(in_x.at[1], -1, 0)
    west = present(in_y.at[0, 1], 0, 1)
    east = present(in_y.at[1, 1], 0, -1)
    low16 = lax.broadcasted_iota(jnp.int32, (16, CELLS), 1) < 64
    west_c = jnp.where(low16, present(in_y.at[0, 2], 1, 1), present(in_y.at[0, 0], -1, 1))
    east_c = jnp.where(low16, present(in_y.at[1, 2], 1, -1), present(in_y.at[1, 0], -1, -1))
    for g in range(GROUPS):
        at = pl.ds(8 * g, 8)
        b, s = g // 4, g % 4
        f_out[1, at, :] = jnp.where(
            low_x,
            roll(north[8 * b : 8 * b + 8], -32 * s),
            roll(south[8 * b : 8 * b + 8], 32 * s),
        )
        b, s = g // 8, g % 8
        for place, w, e in ((2, west, east), (3, west_c, east_c)):
            f_out[place, at, :] = jnp.where(
                low_y,
                roll(w[8 * b : 8 * b + 8], -2 * s),
                roll(e[8 * b : 8 * b + 8], 2 * s),
            )

    halo_x(mate).wait_send()
    halo_y(0, near).wait_send()
    halo_y(mate, near).wait_send()

    @when_far
    def _():
        halo_y(0, far).wait_send()
        halo_y(mate, far).wait_send()

    @when_away
    def _():
        halo_x(away).wait_send()
        halo_y(away, near).wait_send()
        when_far(lambda: halo_y(away, far).wait_send())


def update_kernel(
    f_in,
    obs,
    atm,
    mean_out,
    anom_out,
    state,
    shifted,
    factors,
    result,
    means,
    out_sem,
    mean_sem,
):
    lane8 = lax.broadcasted_iota(jnp.int32, (8, CELLS), 1)
    y8 = lane8 % AY
    first_y, last_y = y8 == 0, y8 == AY - 1
    first_x, last_x = lane8 < AY, lane8 >= CELLS - AY
    groups = range(MEM // 8)

    def at(g):
        return slice(8 * g, 8 * g + 8)

    def shift_all(blocks, wanted):
        out = {}
        turned = {}
        for f in range(4):
            if any((f ^ a) in wanted for a in (0, 1)):
                other = blocks[f ^ 2]
                turned[f, 0] = blocks[f]
                turned[f, 1] = jnp.where(last_y, roll(other, 15), roll(blocks[f], -1))
                turned[f, -1] = jnp.where(first_y, roll(other, -15), roll(blocks[f], 1))
        for f in wanted:
            for dy in (-1, 0, 1):
                own, other = turned[f, dy], turned[f ^ 1, dy]
                out[f, slot(0, dy)] = own
                out[f, slot(1, dy)] = roll(jnp.where(first_x, other, own), -AY)
                out[f, slot(-1, dy)] = roll(jnp.where(last_x, other, own), AY)
        return out

    def allsum(x):
        for step in (4, 2, 1):
            x = x + pltpu.roll(x, step, 0)
        return x

    zero = jnp.zeros((8, CELLS), jnp.float32)
    tapers = [
        max(1.0 - (dx * dx + dy * dy) / 4.0, 0.0) ** 2 / (MEM - 1) for dx, dy in NEAR
    ]

    for batch in range(NB):
        source = f_in if batch == 0 else state
        wanted = (0, 1, 2, 3) if batch == 0 else (0,)
        base = 0 if batch == 0 else 36

        alphas, betas = [], []
        for f in range(4):
            square = zero
            for g in groups:
                block = source[f, at(g), :]
                square = square + block * block
            variance = allsum(square) / (MEM - 1)
            total = [zero, zero, zero]
            for q in range(OB // 8):
                masked = obs[batch, f, 0, at(q), :]
                masked_value = obs[batch, f, 1, at(q), :]
                inverse = 1.0 / (variance + obs[batch, f, 2, at(q), :])
                ratio = obs[batch, f, 3, at(q), :] * inverse
                damping = 1.0 / (1.0 + ratio * lax.rsqrt(ratio))
                weighting = masked * inverse
                total[0] = total[0] + weighting * damping
                total[1] = total[1] + weighting
                total[2] = total[2] + masked_value * inverse
            betas.append(allsum(total[0]))
            alphas.append(allsum(total[2]) - source[f, MEM:, :] * allsum(total[1]))
        alphas = shift_all(alphas, wanted)
        betas = shift_all(betas, wanted)
        alphas = {key: alphas[key] * tapers[key[1]] for key in alphas}
        betas = {key: betas[key] * tapers[key[1]] for key in betas}
        for d in range(9):
            factors[batch, 0, d] = alphas[0, d]
            factors[batch, 1, d] = betas[0, d]

        for g in groups:
            moved = shift_all([source[f, at(g), :] for f in range(4)], wanted)
            for f in wanted:
                for d in range(9):
                    shifted[base + 9 * f + d, at(g), :] = moved[f, d]

        for f in wanted:
            sums = [zero] * 9
            for g in groups:
                block = source[f, at(g), :]
                for d in range(9):
                    sums[d] = sums[d] + shifted[base + 9 * f + d, at(g), :] * block
            sums = [allsum(x) for x in sums]
            mean = source[f, MEM:, :]
            for d in range(9):
                mean = mean + alphas[f, d] * sums[d]
            gains = [betas[f, d] * sums[d] for d in range(9)]
            for g in groups:
                block = source[f, at(g), :]
                for d in range(9):
                    block = block - shifted[base + 9 * f + d, at(g), :] * gains[d]
                if batch + 1 < NB:
                    state[f, at(g), :] = block
                else:
                    result[FIELDS, at(g), :] = block
            if batch + 1 < NB:
                state[f, MEM:, :] = mean
            else:
                means[FIELDS] = mean[:1]

    def sst_copy():
        return pltpu.make_async_copy(result.at[FIELDS], anom_out.at[FIELDS], mean_sem.at[1])

    def field_copy(pair):
        part = pl.ds(2 * pair, 2)
        return pltpu.make_async_copy(result.at[part], anom_out.at[part], out_sem.at[pair])

    sst_copy().start()

    def two_fields(pair, carry):
        fields = (2 * pair, 2 * pair + 1)
        sums = [zero, zero]
        for g in groups:
            for u in range(2):
                sums[u] = sums[u] + atm[fields[u], at(g), :]
        mean = [allsum(x) / MEM for x in sums]
        for batch in range(NB):
            sums = [[zero] * 9, [zero] * 9]
            for g in groups:
                for u in range(2):
                    if batch == 0:
                        block = atm[fields[u], at(g), :] - mean[u]
                        result[fields[u], at(g), :] = block
                    else:
                        block = result[fields[u], at(g), :]
                    for d in range(9):
                        sums[u][d] = sums[u][d] + shifted[36 * batch + d, at(g), :] * block
            sums = [[allsum(x) for x in sums[u]] for u in range(2)]
            for u in range(2):
                for d in range(9):
                    mean[u] = mean[u] + factors[batch, 0, d] * sums[u][d]
            gains = [[factors[batch, 1, d] * sums[u][d] for d in range(9)] for u in range(2)]
            for g in groups:
                for u in range(2):
                    block = result[fields[u], at(g), :]
                    for d in range(9):
                        block = block - shifted[36 * batch + d, at(g), :] * gains[u][d]
                    result[fields[u], at(g), :] = block
        for u in range(2):
            means[fields[u]] = mean[u][:1]
        field_copy(pair).start()
        return carry

    lax.fori_loop(0, FIELDS // 2, two_fields, 0)
    mean_copy = pltpu.make_async_copy(means, mean_out, mean_sem.at[0])
    mean_copy.start()
    sst_copy().wait()
    for pair in range(FIELDS // 2):
        field_copy(pair).wait()
    mean_copy.wait()


def local(
    atm_members,
    ocean_members,
    remap_weights,
    pair_src,
    obs_cell,
    obs_value,
    obs_error,
    obs_live,
    obs_order,
):
    f32 = jnp.float32
    vmem = pl.BlockSpec(memory_space=pltpu.VMEM)
    hbm = pl.BlockSpec(memory_space=pltpu.HBM)
    dma = pltpu.SemaphoreType.DMA
    state, meta = pl.pallas_call(
        exchange_kernel,
        out_shape=(
            jax.ShapeDtypeStruct((4, ROWS, CELLS), f32),
            jax.ShapeDtypeStruct((NB, 4, 4, OB, CELLS), f32),
        ),
        in_specs=[hbm] * 8,
        out_specs=(vmem, vmem),
        scratch_shapes=[
            pltpu.SMEM((1, K), jnp.int32),
            pltpu.VMEM((3, 1, OBS), jnp.int32),
            pltpu.VMEM((2, 1, OBS), f32),
            pltpu.VMEM((9, CHUNKS, MEM, CW), jnp.bfloat16),
            pltpu.VMEM((K, OCN_DEV, CELLS), jnp.bfloat16),
            pltpu.VMEM((MEM, CELLS), f32),
            pltpu.VMEM((CELLS, CELLS), f32),
            pltpu.VMEM((9, 8, CELLS), f32),
            pltpu.VMEM((2, 16, CELLS), f32),
            pltpu.VMEM((2, 24, CELLS), f32),
            pltpu.VMEM((2, 3, 16, CELLS), f32),
            pltpu.VMEM((2, 24, CELLS), f32),
            dma((CHUNKS + 7,)),
            dma((24,)),
            dma((9, CHUNKS)),
            dma((4,)),
            dma((9,)),
            dma((9,)),
            dma((9,)),
        ],
        compiler_params=pltpu.CompilerParams(
            collective_id=0, has_side_effects=True, vmem_limit_bytes=16 * 1024 * 1024
        ),
    )(
        *(
            pltpu.with_memory_space_constraint(x, pltpu.HBM)
            for x in (
                pair_src[0],
                ocean_members[0, 0],
                remap_weights[0, 0],
                obs_cell[0],
                obs_value[0],
                obs_error[0],
                obs_live[0],
                obs_order[0],
            )
        )
    )
    mean, anomaly = pl.pallas_call(
        update_kernel,
        out_shape=(
            jax.ShapeDtypeStruct((COMP, 1, CELLS), f32),
            jax.ShapeDtypeStruct((COMP, MEM, CELLS), f32),
        ),
        in_specs=[vmem] * 3,
        out_specs=(hbm, hbm),
        scratch_shapes=[
            pltpu.VMEM((4, ROWS, CELLS), f32),
            pltpu.VMEM((45, MEM, CELLS), f32),
            pltpu.VMEM((NB, 2, 9, 8, CELLS), f32),
            pltpu.VMEM((COMP, MEM, CELLS), f32),
            pltpu.VMEM((COMP, 1, CELLS), f32),
            dma((FIELDS // 2,)),
            dma((2,)),
        ],
        compiler_params=pltpu.CompilerParams(vmem_limit_bytes=16 * 1024 * 1024),
    )(state, meta, jnp.transpose(atm_members[0, 0], (1, 0, 2)))
    return (mean.reshape(1, 1, COMP, CELLS), jnp.transpose(anomaly, (1, 0, 2))[None, None])


def solution(mesh):
    in_specs = (
        P("gx", "gy", None, None, None),
        P("gx", "gy", None, None),
        P("gx", "gy", None, None, None),
        P("gx", "gy", None),
        P("gx", "gy", None),
        P("gx", "gy", None),
        P("gx", "gy", None),
        P("gx", "gy", None),
        P("gx", "gy", None),
    )
    out_specs = (P("gx", "gy", None, None), P("gx", "gy", None, None, None))
    return jax.shard_map(local, mesh=mesh, in_specs=in_specs, out_specs=out_specs, check_vma=False)
```

```python
import functools

import jax
import jax.numpy as jnp
import numpy as np
from jax import lax
from jax.experimental import pallas as pl
from jax.experimental.pallas import tpu as pltpu
from jax.sharding import PartitionSpec as P

MEM = 80
AX = 8
AY = 16
OCN_DEV = 1024
OB = 32
NB = 2
K = 4
FIELDS = 12
COMP = 13
CELLS = 128
OBS = 64
ROWS = 88
GROUPS = 11
CHUNKS = 4
CW = OCN_DEV // CHUNKS
FIRST, SECOND, THIRD, BOTH, WHOLE = (0, 1), (1, 1), (2, 2), (0, 2), (0, 4)

MESH = pl.DeviceIdType.MESH
NEAR = [(dx, dy) for dx in (-1, 0, 1) for dy in (-1, 0, 1)]
AROUND = [d for d in NEAR if d != (0, 0)]


def build_tables():
    ring_e, ring_r, gathered = {}, {}, np.zeros(CELLS, np.int32)
    middle = {0: 32, 1: 64}
    for x in range(-2, AX + 2):
        for y in range(-2, AY + 2):
            out_x, out_y = not 0 <= x < AX, not 0 <= y < AY
            if not (out_x or out_y):
                continue
            lane = (x % AX) * AY + y % AY
            if out_y:
                gathered[middle[out_x]] = lane
                lane = middle[out_x]
                middle[out_x] += 1
            ring_e[x, y] = lane
            if -1 <= x <= AX and -1 <= y <= AY:
                ring_r[x, y] = len(ring_r)

    def code(x, y, ring):
        inside = 0 <= x < AX and 0 <= y < AY
        return x * AY + y if inside else CELLS + ring[x, y]

    shifts = np.zeros((28, CELLS), np.int32)
    for d, (dx, dy) in enumerate(NEAR):
        for c in range(CELLS):
            x, y = c // AY + dx, c % AY + dy
            shifts[d, c] = code(x, y, ring_e)
            shifts[18 + d, c] = code(x, y, ring_r)
        for (x, y), lane in ring_r.items():
            shifts[9 + d, lane] = code(x + dx, y + dy, ring_e)
    shifts[27] = gathered
    owners = np.full((8, CELLS), -1, np.int32)
    for n, ring in enumerate((ring_e, ring_r)):
        for (x, y), lane in ring.items():
            owners[2 * n, lane] = (x % AX) * AY + y % AY
            owners[2 * n + 1, lane] = slot(x // AX, y // AY)
    return np.repeat(shifts[:, None], 8, axis=1), owners


def slot(dx, dy):
    return (dx + 1) * 3 + dy + 1


def roll(x, shift):
    shift = shift % CELLS
    return x if shift == 0 else pltpu.roll(x, shift, 1)


def exchange_kernel(
    src_hbm,
    ocean,
    weights,
    cell_hbm,
    value_hbm,
    error_hbm,
    live_hbm,
    order_hbm,
    owners_hbm,
    f_out,
    obs_out,
    src,
    owners,
    ints,
    floats,
    oce,
    wv,
    acc,
    columns,
    meta_in,
    pack_y,
    pack_x,
    in_y,
    in_x,
    local_sem,
    oce_send,
    oce_recv,
    meta_send,
    meta_recv,
    halo_send,
    halo_recv,
):
    i = lax.axis_index("gx")
    j = lax.axis_index("gy")
    nx = lax.axis_size("gx")
    ny = lax.axis_size("gy")

    away = 2 * (i % 2) - 1
    mate = -away
    has_away = jnp.logical_and(i + away >= 0, i + away < nx)
    near = 1 - 2 * ((j % 4 + 3) // 4)
    far = -near
    has_far = jnp.logical_and(j + far >= 0, j + far < ny)
    when_away, when_far = pl.when(has_away), pl.when(has_far)

    def has(dx, dy):
        cond = None
        for pos, step, count in ((i, dx, nx), (j, dy, ny)):
            if step:
                ok = (pos > 0) if step < 0 else (pos < count - 1)
                cond = ok if cond is None else jnp.logical_and(cond, ok)
        return cond

    def when(dx, dy):
        return pl.when(has(dx, dy))

    def device(dx, dy):
        return (i + dx, j + dy)

    own_load = [
        pltpu.make_async_copy(
            ocean.at[:, pl.ds(c * CW, CW)], oce.at[4, c], local_sem.at[c]
        )
        for c in range(CHUNKS)
    ]
    for copy in own_load:
        copy.start()

    barrier = pltpu.get_barrier_semaphore()

    def greet(dx, dy):
        pl.semaphore_signal(barrier, inc=1, device_id=device(dx, dy), device_id_type=MESH)

    @when_far
    def _():
        greet(0, far)

    greet(0, near)

    @when_away
    def _():
        greet(away, 0)

    greet(mate, 0)

    pl.semaphore_wait(
        barrier,
        2 + has_away.astype(jnp.int32) + has_far.astype(jnp.int32),
    )

    def tile(p, piece):
        return oce.at[p, pl.ds(*piece)]

    def ocean_copy(piece, from_dx, from_dy, dx, dy, sem):
        target = slot(from_dx - dx, from_dy - dy)
        return pltpu.make_async_remote_copy(
            src_ref=tile(slot(from_dx, from_dy), piece),
            dst_ref=tile(target, piece),
            send_sem=oce_send.at[sem],
            recv_sem=oce_recv.at[target, piece[0]],
            device_id=device(dx, dy),
            device_id_type=MESH,
        )

    def arrived(piece, dx, dy):
        ocean_copy(piece, 0, 0, -dx, -dy, 0).wait_recv()

    def meta_copy(dx, dy, sem):
        if isinstance(dx, int):
            source, target = meta_in.at[4], meta_in.at[slot(0, -dy)]
            recv = meta_recv.at[slot(0, -dy)]
        else:
            source, target = meta_in.at[pl.ds(3, 3)], meta_in.at[pl.ds(slot(-dx, -1), 3)]
            recv = meta_recv.at[slot(-dx, 0)]
        return pltpu.make_async_remote_copy(
            src_ref=source,
            dst_ref=target,
            send_sem=meta_send.at[sem],
            recv_sem=recv,
            device_id=device(dx, dy),
            device_id_type=MESH,
        )

    sends = []

    def send(far_needed, away_needed, *spec):
        sends.append((far_needed, away_needed, spec + (len(sends),)))
        ocean_copy(*sends[-1][2]).start()

    for c in range(CHUNKS):
        own_load[c].wait()
        if c == 0:
            send(False, False, FIRST, 0, 0, 0, near)
            when_far(lambda: send(True, False, FIRST, 0, 0, 0, far))
        if c == 1:
            send(False, False, SECOND, 0, 0, 0, near)
            when_far(lambda: send(True, False, SECOND, 0, 0, 0, far))
        if c == 3:

            @when_away
            def _():
                send(False, True, THIRD, 0, 0, away, 0)
                send(False, True, BOTH, 0, 0, away, 0)

            send(False, False, THIRD, 0, 0, 0, near)
            when_far(lambda: send(True, False, THIRD, 0, 0, 0, far))
            send(False, False, WHOLE, 0, 0, mate, 0)

    small_load = [
        pltpu.make_async_copy(source, target, local_sem.at[CHUNKS + 1 + n])
        for n, (source, target) in enumerate(
            (
                (cell_hbm, ints.at[0]),
                (live_hbm, ints.at[1]),
                (order_hbm, ints.at[2]),
                (value_hbm, floats.at[0]),
                (error_hbm, floats.at[1]),
                (src_hbm, src),
                (owners_hbm, owners),
            )
        )
    ]
    for copy in small_load:
        copy.start()
    w_load = pltpu.make_async_copy(weights, wv, local_sem.at[CHUNKS])
    w_load.start()

    for copy in small_load:
        copy.wait()
    lane = lax.broadcasted_iota(jnp.int32, (OBS, OBS), 0)
    perm = jnp.where(lane == ints[2], 1.0, 0.0)
    rows = [
        ints[0].astype(jnp.float32),
        floats[0],
        floats[1],
        ints[1].astype(jnp.float32),
    ]
    stacked = jnp.concatenate(rows + [jnp.zeros((4, OBS), jnp.float32)], axis=0)
    ordered = jnp.dot(
        stacked,
        perm,
        precision=lax.Precision.HIGHEST,
        preferred_element_type=jnp.float32,
    )
    meta_in[4] = jnp.concatenate([ordered, jnp.zeros((8, CELLS - OBS), jnp.float32)], axis=1)

    @pl.when(jnp.logical_not(has_far))
    def _():
        meta_in[slot(0, far)] = jnp.zeros((8, CELLS), jnp.float32)


    positions = [
        (src[0, k] // ny - i + 1) * 3 + (src[0, k] % ny - j + 1) for k in range(K)
    ]

    def product(dx, dy, c):
        p = slot(dx, dy)
        which = jnp.int32(0)
        valid = positions[0] == p
        for k in range(1, K):
            which = jnp.where(positions[k] == p, k, which)
            valid = jnp.logical_or(valid, positions[k] == p)
        part = jnp.dot(
            oce[p, c],
            wv[which, pl.ds(c * CW, CW), :],
            preferred_element_type=jnp.float32,
        )
        return jnp.where(valid, part, 0.0)

    w_load.wait()
    total = product(0, 0, 0)
    for c in range(1, CHUNKS):
        total = total + product(0, 0, c)
    acc[...] = total

    def add(dx, dy, piece):
        for c in range(piece[0], piece[0] + piece[1]):
            acc[...] += product(dx, dy, c)

    def from_y(piece, with_away):
        def one(dy, is_far):
            arrived(piece, 0, dy)
            send(is_far, False, piece, 0, dy, mate, 0)
            if with_away:
                when_away(lambda: send(is_far, True, piece, 0, dy, away, 0))

        one(near, False)
        when_far(lambda: one(far, True))

    from_y(FIRST, True)
    meta_copy(0, near, 0).start()
    when_far(lambda: meta_copy(0, far, 1).start())

    @when_away
    def _():
        arrived(THIRD, away, 0)
        send(False, True, THIRD, away, 0, 0, near)
        when_far(lambda: send(True, True, THIRD, away, 0, 0, far))

    from_y(SECOND, True)
    arrived(WHOLE, mate, 0)
    add(mate, 0, WHOLE)
    add(0, near, BOTH)
    when_far(lambda: add(0, far, BOTH))
    when_away(lambda: add(away, 0, THIRD))
    from_y(THIRD, False)
    add(0, near, THIRD)
    when_far(lambda: add(0, far, THIRD))

    meta_copy(0, -near, 0).wait_recv()
    when_far(lambda: meta_copy(0, -far, 1).wait_recv())
    meta_copy(mate, 0, 2).start()
    when_away(lambda: meta_copy(away, 0, 3).start())

    @when_away
    def _():
        arrived(BOTH, away, 0)
        add(away, 0, BOTH)

    def corner(dx, dy, piece):
        arrived(piece, dx, dy)
        add(dx, dy, piece)

    for piece in (FIRST, SECOND, THIRD):
        corner(mate, near, piece)
        when_far(lambda: corner(mate, far, piece))

    for piece in (FIRST, SECOND, THIRD):

        @when_away
        def _():
            corner(away, near, piece)
            when_far(lambda: corner(away, far, piece))

    sst = acc[...]
    mean = jnp.sum(sst, axis=0, keepdims=True) / MEM
    anomaly = sst - mean
    pieces = [anomaly[8 * g : 8 * g + 8] for g in range(MEM // 8)]
    pieces.append(jnp.broadcast_to(mean, (8, CELLS)))
    lane8 = lax.broadcasted_iota(jnp.int32, (8, CELLS), 1)
    pair = (lane8 % AY) // 2
    quarter = lane8 // 32

    for block in range(2):
        west = jnp.zeros((8, CELLS), jnp.float32)
        east = west
        for g in range(8 * block, min(8 * block + 8, GROUPS)):
            s = g % 8
            west = jnp.where(pair == s, roll(pieces[g], 2 * s), west)
            east = jnp.where(pair == 7 - s, roll(pieces[g], -2 * s), east)
        pack_y[0, 8 * block : 8 * block + 8, :] = west
        pack_y[1, 8 * block : 8 * block + 8, :] = east
    for block in range(3):
        north = jnp.zeros((8, CELLS), jnp.float32)
        south = north
        for g in range(4 * block, min(4 * block + 4, GROUPS)):
            s = g % 4
            north = jnp.where(quarter == s, roll(pieces[g], 32 * s), north)
            south = jnp.where(quarter == 3 - s, roll(pieces[g], -32 * s), south)
        pack_x[0, 8 * block : 8 * block + 8, :] = north
        pack_x[1, 8 * block : 8 * block + 8, :] = south

    def halo_y(dx, dy):
        side = (dy + 1) // 2
        return pltpu.make_async_remote_copy(
            src_ref=pack_y.at[side],
            dst_ref=in_y.at[side, 1 - dx],
            send_sem=halo_send.at[slot(dx, dy)],
            recv_sem=halo_recv.at[slot(-dx, -dy)],
            device_id=device(dx, dy),
            device_id_type=MESH,
        )

    def halo_x(dx):
        side = (dx + 1) // 2
        return pltpu.make_async_remote_copy(
            src_ref=pack_x.at[side],
            dst_ref=in_x.at[side],
            send_sem=halo_send.at[slot(dx, 0)],
            recv_sem=halo_recv.at[slot(-dx, 0)],
            device_id=device(dx, 0),
            device_id_type=MESH,
        )

    @when_away
    def _():
        when_far(lambda: halo_y(away, far).start())
        halo_y(away, near).start()

    @when_far
    def _():
        halo_y(mate, far).start()
        halo_y(0, far).start()

    halo_y(mate, near).start()
    halo_y(0, near).start()
    when_away(lambda: halo_x(away).start())
    halo_x(mate).start()

    f_out[0, :MEM, :] = anomaly
    f_out[0, MEM:, :] = pieces[-1]

    absent = jnp.where(lax.broadcasted_iota(jnp.int32, (8, CELLS), 0) == 2, 1.0, 0.0)
    meta_copy(-mate, 0, 2).wait_recv()
    when_away(lambda: meta_copy(-away, 0, 3).wait_recv())

    blocks = []
    for dx, dy in NEAR:
        if (dx, dy) == (0, 0):
            blocks.append(meta_in[4])
        else:
            blocks.append(jnp.where(has(dx, dy), meta_in[slot(dx, dy)], absent))
    blocks.append(jnp.zeros((CELLS - 72, CELLS), jnp.float32))
    columns[...] = jnp.concatenate(blocks, axis=0).T

    lane32 = lax.broadcasted_iota(jnp.int32, (OB, CELLS), 1)
    for batch in range(NB):
        rows = slice(batch * OB, (batch + 1) * OB)

        def dense(dx, dy, lanes):
            at = 8 * slot(dx, dy)
            cells, values, errors, alive = (
                jnp.broadcast_to(columns[rows, at + n : at + n + 1], (OB, CELLS))
                for n in range(4)
            )
            hit = jnp.where(cells == lanes, alive, 0.0)
            return hit, hit * values, errors + (1.0 - alive), errors

        cell_row = jnp.broadcast_to(owners[2 * batch : 2 * batch + 1, :], (OB, CELLS))
        tile_row = jnp.broadcast_to(owners[2 * batch + 1 : 2 * batch + 2, :], (OB, CELLS))
        cell_row = cell_row.astype(jnp.float32)
        around = dense(-1, -1, cell_row)
        for dx, dy in AROUND[1:]:
            other = dense(dx, dy, cell_row)
            chosen = tile_row == slot(dx, dy)
            around = tuple(jnp.where(chosen, n, o) for n, o in zip(other, around))
        for place, parts in enumerate((dense(0, 0, lane32.astype(jnp.float32)), around)):
            for n, part in enumerate(parts):
                obs_out[batch, place, n] = part

    def finish(far_needed, away_needed):
        for f, a, spec in sends:
            if (f, a) == (far_needed, away_needed):
                ocean_copy(*spec).wait_send()

    finish(False, False)
    meta_copy(0, near, 0).wait_send()
    meta_copy(mate, 0, 2).wait_send()

    @when_far
    def _():
        finish(True, False)
        meta_copy(0, far, 1).wait_send()

    @when_away
    def _():
        finish(False, True)
        meta_copy(away, 0, 3).wait_send()
        when_far(lambda: finish(True, True))

    halo_x(-mate).wait_recv()
    halo_y(0, -near).wait_recv()
    halo_y(-mate, -near).wait_recv()

    @when_far
    def _():
        halo_y(0, -far).wait_recv()
        halo_y(-mate, -far).wait_recv()

    @when_away
    def _():
        halo_x(-away).wait_recv()
        halo_y(-away, -near).wait_recv()
        when_far(lambda: halo_y(-away, -far).wait_recv())

    low_y = (lane8 % AY) < 8
    low_x = lane8 < 64
    zero = jnp.zeros((8, CELLS), jnp.float32)

    def present(ref, dx, dy):
        return jnp.where(has(dx, dy), ref[...], 0.0)

    north = present(in_x.at[0], 1, 0)
    south = present(in_x.at[1], -1, 0)
    west = present(in_y.at[0, 1], 0, 1)
    east = present(in_y.at[1, 1], 0, -1)
    low16 = lax.broadcasted_iota(jnp.int32, (16, CELLS), 1) < 64
    west_c = jnp.where(low16, present(in_y.at[0, 2], 1, 1), present(in_y.at[0, 0], -1, 1))
    east_c = jnp.where(low16, present(in_y.at[1, 2], 1, -1), present(in_y.at[1, 0], -1, -1))
    for g in range(GROUPS):
        at = pl.ds(8 * g, 8)
        b, s = g // 4, g % 4
        f_out[1, at, :] = jnp.where(
            low_x,
            roll(north[8 * b : 8 * b + 8], -32 * s),
            roll(south[8 * b : 8 * b + 8], 32 * s),
        )
        b, s = g // 8, g % 8
        for place, w, e in ((2, west, east), (3, west_c, east_c)):
            f_out[place, at, :] = jnp.where(
                low_y,
                roll(w[8 * b : 8 * b + 8], -2 * s),
                roll(e[8 * b : 8 * b + 8], 2 * s),
            )

    halo_x(mate).wait_send()
    halo_y(0, near).wait_send()
    halo_y(mate, near).wait_send()

    @when_far
    def _():
        halo_y(0, far).wait_send()
        halo_y(mate, far).wait_send()

    @when_away
    def _():
        halo_x(away).wait_send()
        halo_y(away, near).wait_send()
        when_far(lambda: halo_y(away, far).wait_send())


def update_kernel(
    f_in,
    obs,
    tables,
    atm,
    mean_out,
    anom_out,
    around,
    state,
    first_shifts,
    other_shifts,
    second_shifts,
    factors,
    covariance,
    result,
    field_mean,
    means,
    out_sem,
    mean_sem,
):
    lane8 = lax.broadcasted_iota(jnp.int32, (8, CELLS), 1)
    groups = range(MEM // 8)
    pairs = FIELDS // 2
    always = lax.axis_index("gx") >= 0

    def at(g):
        return slice(8 * g, 8 * g + 8)

    def take(block, lanes):
        return jnp.take_along_axis(block, lanes, axis=1, mode="promise_in_bounds")

    def shift(base, d, own, ring):
        if d == 4 and base != 9:
            return own
        table = tables[base + d]
        lanes = jnp.bitwise_and(table, CELLS - 1)
        if d == 4:
            return take(ring, lanes)
        return jnp.where(table >= CELLS, take(ring, lanes), take(own, lanes))

    def allsum(x):
        for step in (4, 2, 1):
            x = x + pltpu.roll(x, step, 0)
        return x

    zero = jnp.zeros((8, CELLS), jnp.float32)
    tapers = [
        max(1.0 - (dx * dx + dy * dy) / 4.0, 0.0) ** 2 / (MEM - 1) for dx, dy in NEAR
    ]

    def observe(batch, sources, bases):
        alphas, betas = [], []
        for f, source in enumerate(sources):
            square = zero
            for g in groups:
                block = source[at(g), :]
                square = square + block * block
            variance = allsum(square) / (MEM - 1)
            total = [zero, zero, zero]
            for q in range(OB // 8):
                masked = obs[batch, f, 0, at(q), :]
                masked_value = obs[batch, f, 1, at(q), :]
                inverse = 1.0 / (variance + obs[batch, f, 2, at(q), :])
                ratio = obs[batch, f, 3, at(q), :] * inverse
                damping = 1.0 / (1.0 + ratio * lax.rsqrt(ratio))
                weighting = masked * inverse
                total[0] = total[0] + weighting * damping
                total[1] = total[1] + weighting
                total[2] = total[2] + masked_value * inverse
            betas.append(allsum(total[0]))
            alphas.append(allsum(total[2]) - source[MEM:, :] * allsum(total[1]))
        for base in bases:
            for kind, blocks in enumerate((alphas, betas)):
                for d in range(9):
                    factors[kind, base + d] = shift(base, d, *blocks) * tapers[d]

    def shift_groups(base, target, own, ring, chosen):
        for g in chosen:
            for d in range(9):
                target[d, at(g), :] = shift(base, d, own[at(g), :], ring[at(g), :])

    def sst_step(base, source, mean, shifts, store):
        sums = [zero] * 9
        for g in groups:
            block = source[at(g), :]
            for d in range(9):
                sums[d] = sums[d] + shifts[d, at(g), :] * block
        sums = [allsum(x) for x in sums]
        for d in range(9):
            mean = mean + factors[0, base + d] * sums[d]
        gains = [factors[1, base + d] * sums[d] for d in range(9)]
        for g in groups:
            block = source[at(g), :]
            for d in range(9):
                block = block - shifts[d, at(g), :] * gains[d]
            store[at(g), :] = block
        return mean

    def field_step(base, shifted, fields, sums):
        mean = [field_mean[u] for u in fields]
        for n, u in enumerate(fields):
            for d in range(9):
                mean[n] = mean[n] + factors[0, base + d] * sums[n][d]
        gains = [[factors[1, base + d] * sums[n][d] for d in range(9)] for n in range(2)]
        for g in groups:
            for n, u in enumerate(fields):
                block = result[u, at(g), :]
                for d in range(9):
                    block = block - shifted[d, at(g), :] * gains[n][d]
                result[u, at(g), :] = block
        return mean

    gathered = tables[27]
    edge = jnp.logical_or(lane8 < 32, lane8 >= 96)
    for g in range(GROUPS):
        middle = jnp.where(
            lane8 < 64, take(f_in[2, at(g), :], gathered), take(f_in[3, at(g), :], gathered)
        )
        around[at(g), :] = jnp.where(edge, f_in[1, at(g), :], middle)
    own = f_in.at[0]
    shift_groups(0, first_shifts, own, around, groups)
    observe(0, (own, around), (0, 9))

    def first_covariance(pair):
        fields = (2 * pair, 2 * pair + 1)
        total = [zero, zero]
        for g in groups:
            for n, u in enumerate(fields):
                total[n] = total[n] + atm[u, at(g), :]
        mean = [allsum(x) / MEM for x in total]
        sums = [[zero] * 9, [zero] * 9]
        for g in groups:
            for n, u in enumerate(fields):
                block = atm[u, at(g), :] - mean[n]
                result[u, at(g), :] = block
                for d in range(9):
                    sums[n][d] = sums[n][d] + first_shifts[d, at(g), :] * block
        for n, u in enumerate(fields):
            field_mean[u] = mean[n]
            for d in range(9):
                covariance[u, d] = allsum(sums[n][d])
        shift_groups(9, other_shifts, own, around, groups[2 * pair : 2 * pair + 2])

    for pair in range(pairs):
        pl.when(always)(functools.partial(first_covariance, pair))
    state[0, MEM:, :] = sst_step(0, own, own[MEM:, :], first_shifts, state.at[0])
    mean = shift(9, 4, own[MEM:, :], around[MEM:, :])
    state[1, MEM:, :] = sst_step(9, other_shifts.at[4], mean, other_shifts, state.at[1])
    observe(1, (state.at[0], state.at[1]), (18,))

    def first_update(pair):
        fields = (2 * pair, 2 * pair + 1)
        sums = [[covariance[u, d] for d in range(9)] for u in fields]
        mean = field_step(0, first_shifts, fields, sums)
        for n, u in enumerate(fields):
            field_mean[u] = mean[n]
        shift_groups(
            18, second_shifts, state.at[0], state.at[1], groups[2 * pair : 2 * pair + 2]
        )

    for pair in range(pairs):
        pl.when(always)(functools.partial(first_update, pair))
    mean = sst_step(18, state.at[0], state[0, MEM:, :], second_shifts, result.at[FIELDS])
    means[FIELDS] = mean[:1]
    sst_copy = pltpu.make_async_copy(result.at[FIELDS], anom_out.at[FIELDS], mean_sem.at[1])
    sst_copy.start()

    def field_copy(pair):
        part = pl.ds(2 * pair, 2)
        return pltpu.make_async_copy(result.at[part], anom_out.at[part], out_sem.at[pair])

    def second_batch(pair):
        fields = (2 * pair, 2 * pair + 1)
        sums = [[zero] * 9, [zero] * 9]
        for g in groups:
            for n, u in enumerate(fields):
                block = result[u, at(g), :]
                for d in range(9):
                    sums[n][d] = sums[n][d] + second_shifts[d, at(g), :] * block
        sums = [[allsum(x) for x in sums[n]] for n in range(2)]
        mean = field_step(18, second_shifts, fields, sums)
        for n, u in enumerate(fields):
            means[u] = mean[n][:1]
        field_copy(pair).start()

    for pair in range(pairs):
        pl.when(always)(functools.partial(second_batch, pair))
    mean_copy = pltpu.make_async_copy(means, mean_out, mean_sem.at[0])
    mean_copy.start()
    sst_copy.wait()
    for pair in range(pairs):
        field_copy(pair).wait()
    mean_copy.wait()


def local(
    atm_members,
    ocean_members,
    remap_weights,
    pair_src,
    obs_cell,
    obs_value,
    obs_error,
    obs_live,
    obs_order,
):
    f32 = jnp.float32
    shifts, owners = build_tables()
    vmem = pl.BlockSpec(memory_space=pltpu.VMEM)
    hbm = pl.BlockSpec(memory_space=pltpu.HBM)
    dma = pltpu.SemaphoreType.DMA
    state, tables = pl.pallas_call(
        exchange_kernel,
        out_shape=(
            jax.ShapeDtypeStruct((4, ROWS, CELLS), f32),
            jax.ShapeDtypeStruct((NB, 2, 4, OB, CELLS), f32),
        ),
        in_specs=[hbm] * 9,
        out_specs=(vmem, vmem),
        scratch_shapes=[
            pltpu.SMEM((1, K), jnp.int32),
            pltpu.VMEM((8, CELLS), jnp.int32),
            pltpu.VMEM((3, 1, OBS), jnp.int32),
            pltpu.VMEM((2, 1, OBS), f32),
            pltpu.VMEM((9, CHUNKS, MEM, CW), jnp.bfloat16),
            pltpu.VMEM((K, OCN_DEV, CELLS), jnp.bfloat16),
            pltpu.VMEM((MEM, CELLS), f32),
            pltpu.VMEM((CELLS, CELLS), f32),
            pltpu.VMEM((9, 8, CELLS), f32),
            pltpu.VMEM((2, 16, CELLS), f32),
            pltpu.VMEM((2, 24, CELLS), f32),
            pltpu.VMEM((2, 3, 16, CELLS), f32),
            pltpu.VMEM((2, 24, CELLS), f32),
            dma((CHUNKS + 8,)),
            dma((24,)),
            dma((9, CHUNKS)),
            dma((4,)),
            dma((9,)),
            dma((9,)),
            dma((9,)),
        ],
        compiler_params=pltpu.CompilerParams(
            collective_id=0, has_side_effects=True, vmem_limit_bytes=16 * 1024 * 1024
        ),
    )(
        *(
            pltpu.with_memory_space_constraint(x, pltpu.HBM)
            for x in (
                pair_src[0],
                ocean_members[0, 0],
                remap_weights[0, 0],
                obs_cell[0],
                obs_value[0],
                obs_error[0],
                obs_live[0],
                obs_order[0],
                jnp.asarray(owners),
            )
        )
    )
    mean, anomaly = pl.pallas_call(
        update_kernel,
        out_shape=(
            jax.ShapeDtypeStruct((COMP, 1, CELLS), f32),
            jax.ShapeDtypeStruct((COMP, MEM, CELLS), f32),
        ),
        in_specs=[vmem] * 4,
        out_specs=(hbm, hbm),
        scratch_shapes=[
            pltpu.VMEM((ROWS, CELLS), f32),
            pltpu.VMEM((2, ROWS, CELLS), f32),
            pltpu.VMEM((9, MEM, CELLS), f32),
            pltpu.VMEM((9, MEM, CELLS), f32),
            pltpu.VMEM((9, MEM, CELLS), f32),
            pltpu.VMEM((2, 27, 8, CELLS), f32),
            pltpu.VMEM((FIELDS, 9, 8, CELLS), f32),
            pltpu.VMEM((COMP, MEM, CELLS), f32),
            pltpu.VMEM((FIELDS, 8, CELLS), f32),
            pltpu.VMEM((COMP, 1, CELLS), f32),
            dma((FIELDS // 2,)),
            dma((2,)),
        ],
        compiler_params=pltpu.CompilerParams(vmem_limit_bytes=16 * 1024 * 1024),
    )(state, tables, jnp.asarray(shifts), jnp.transpose(atm_members[0, 0], (1, 0, 2)))
    return (mean.reshape(1, 1, COMP, CELLS), jnp.transpose(anomaly, (1, 0, 2))[None, None])


def solution(mesh):
    in_specs = (
        P("gx", "gy", None, None, None),
        P("gx", "gy", None, None),
        P("gx", "gy", None, None, None),
        P("gx", "gy", None),
        P("gx", "gy", None),
        P("gx", "gy", None),
        P("gx", "gy", None),
        P("gx", "gy", None),
        P("gx", "gy", None),
    )
    out_specs = (P("gx", "gy", None, None), P("gx", "gy", None, None, None))
    return jax.shard_map(local, mesh=mesh, in_specs=in_specs, out_specs=out_specs, check_vma=False)
```

```python
import functools

import jax
import jax.numpy as jnp
import numpy as np
from jax import lax
from jax.experimental import pallas as pl
from jax.experimental.pallas import tpu as pltpu
from jax.sharding import PartitionSpec as P

MEM = 80
AX = 8
AY = 16
OCN_DEV = 1024
OB = 32
NB = 2
K = 4
FIELDS = 12
COMP = 13
CELLS = 128
OBS = 64
ROWS = 88
GROUPS = 11
CHUNKS = 4
CW = OCN_DEV // CHUNKS
FIRST, SECOND, THIRD, BOTH, WHOLE = (0, 1), (1, 1), (2, 2), (0, 2), (0, 4)

MESH = pl.DeviceIdType.MESH
NEAR = [(dx, dy) for dx in (-1, 0, 1) for dy in (-1, 0, 1)]
AROUND = [d for d in NEAR if d != (0, 0)]


def build_tables():
    ring_e, ring_r, gathered = {}, {}, np.zeros(CELLS, np.int32)
    middle = {0: 32, 1: 64}
    for x in range(-2, AX + 2):
        for y in range(-2, AY + 2):
            out_x, out_y = not 0 <= x < AX, not 0 <= y < AY
            if not (out_x or out_y):
                continue
            lane = (x % AX) * AY + y % AY
            if out_y:
                gathered[middle[out_x]] = (lane + 4 * out_x) % CELLS
                lane = middle[out_x]
                middle[out_x] += 1
            ring_e[x, y] = lane
            if -1 <= x <= AX and -1 <= y <= AY:
                ring_r[x, y] = len(ring_r)

    def code(x, y, ring):
        inside = 0 <= x < AX and 0 <= y < AY
        return x * AY + y if inside else CELLS + ring[x, y]

    shifts = np.zeros((28, CELLS), np.int32)
    for d, (dx, dy) in enumerate(NEAR):
        for c in range(CELLS):
            x, y = c // AY + dx, c % AY + dy
            shifts[d, c] = code(x, y, ring_e)
            shifts[18 + d, c] = code(x, y, ring_r)
        for (x, y), lane in ring_r.items():
            shifts[9 + d, lane] = code(x + dx, y + dy, ring_e)
    shifts[27] = gathered
    owners = np.full((8, CELLS), -1, np.int32)
    for n, ring in enumerate((ring_e, ring_r)):
        for (x, y), lane in ring.items():
            owners[2 * n, lane] = (x % AX) * AY + y % AY
            owners[2 * n + 1, lane] = slot(x // AX, y // AY)
    return np.repeat(shifts[:, None], 8, axis=1), owners


def slot(dx, dy):
    return (dx + 1) * 3 + dy + 1


def home(dx, dy):
    return (dx + 1) * 3 + (2 if isinstance(dy, int) and dy == 0 else (dy + 1) // 2)


def roll(x, shift):
    shift = shift % CELLS
    return x if shift == 0 else pltpu.roll(x, shift, 1)


def exchange_kernel(
    src_hbm,
    ocean,
    weights,
    cell_hbm,
    value_hbm,
    error_hbm,
    live_hbm,
    order_hbm,
    owners_hbm,
    f_out,
    own_shifts,
    obs_out,
    src,
    owners,
    ints,
    floats,
    oce,
    wv,
    acc,
    columns,
    meta_in,
    pack_y,
    pack_x,
    in_y,
    in_x,
    local_sem,
    oce_send,
    oce_recv,
    both_send,
    both_recv,
    meta_send,
    meta_recv,
    halo_send,
    halo_recv,
):
    i = lax.axis_index("gx")
    j = lax.axis_index("gy")
    nx = lax.axis_size("gx")
    ny = lax.axis_size("gy")

    away = 2 * (i % 2) - 1
    mate = -away
    has_away = jnp.logical_and(i + away >= 0, i + away < nx)
    near = 1 - 2 * ((j % 4 + 3) // 4)
    far = -near
    has_far = jnp.logical_and(j + far >= 0, j + far < ny)
    when_away, when_far = pl.when(has_away), pl.when(has_far)
    when_no_far = pl.when(jnp.logical_not(has_far))

    def has(dx, dy):
        cond = None
        for pos, step, count in ((i, dx, nx), (j, dy, ny)):
            if step:
                ok = (pos > 0) if step < 0 else (pos < count - 1)
                cond = ok if cond is None else jnp.logical_and(cond, ok)
        return cond

    def when(dx, dy):
        return pl.when(has(dx, dy))

    def device(dx, dy):
        return (i + dx, j + dy)

    own_load = [
        pltpu.make_async_copy(
            ocean.at[:, pl.ds(c * CW, CW)], oce.at[home(0, 0), c], local_sem.at[c]
        )
        for c in range(CHUNKS)
    ]
    for copy in own_load:
        copy.start()

    barrier = pltpu.get_barrier_semaphore()

    def greet(dx, dy):
        pl.semaphore_signal(barrier, inc=1, device_id=device(dx, dy), device_id_type=MESH)

    @when_far
    def _():
        greet(0, far)

    greet(0, near)

    @when_away
    def _():
        greet(away, 0)

    greet(mate, 0)

    pl.semaphore_wait(
        barrier,
        2 + has_away.astype(jnp.int32) + has_far.astype(jnp.int32),
    )

    def tile(p, piece):
        return oce.at[p, pl.ds(*piece)]

    def ocean_copy(piece, from_dx, from_dy, dx, dy, sem):
        target = home(from_dx - dx, from_dy - dy)
        return pltpu.make_async_remote_copy(
            src_ref=tile(home(from_dx, from_dy), piece),
            dst_ref=tile(target, piece),
            send_sem=oce_send.at[sem],
            recv_sem=oce_recv.at[target, piece[0]],
            device_id=device(dx, dy),
            device_id_type=MESH,
        )

    def arrived(piece, dx, dy):
        ocean_copy(piece, 0, 0, -dx, -dy, 0).wait_recv()

    def both_copy(piece, dx, sem):
        target = home(-dx, -1)
        return pltpu.make_async_remote_copy(
            src_ref=oce.at[pl.ds(home(0, -1), 2), pl.ds(*piece)],
            dst_ref=oce.at[pl.ds(target, 2), pl.ds(*piece)],
            send_sem=both_send.at[sem],
            recv_sem=both_recv.at[sem],
            device_id=device(dx, 0),
            device_id_type=MESH,
        )

    def meta_copy(dx, dy, sem):
        if isinstance(dx, int):
            source, target = meta_in.at[4], meta_in.at[slot(0, -dy)]
            recv = meta_recv.at[slot(0, -dy)]
        else:
            source, target = meta_in.at[pl.ds(3, 3)], meta_in.at[pl.ds(slot(-dx, -1), 3)]
            recv = meta_recv.at[slot(-dx, 0)]
        return pltpu.make_async_remote_copy(
            src_ref=source,
            dst_ref=target,
            send_sem=meta_send.at[sem],
            recv_sem=recv,
            device_id=device(dx, dy),
            device_id_type=MESH,
        )

    sends = []

    def send(far_needed, away_needed, *spec):
        sends.append((far_needed, away_needed, spec + (len(sends),)))
        ocean_copy(*sends[-1][2]).start()

    for c in range(CHUNKS):
        own_load[c].wait()
        if c == 0:
            send(False, False, FIRST, 0, 0, 0, near)
            when_far(lambda: send(True, False, FIRST, 0, 0, 0, far))
        if c == 1:
            send(False, False, SECOND, 0, 0, 0, near)
            when_far(lambda: send(True, False, SECOND, 0, 0, 0, far))
        if c == 3:

            @when_away
            def _():
                send(False, True, THIRD, 0, 0, away, 0)
                send(False, True, BOTH, 0, 0, away, 0)

            send(False, False, THIRD, 0, 0, 0, near)
            when_far(lambda: send(True, False, THIRD, 0, 0, 0, far))
            send(False, False, WHOLE, 0, 0, mate, 0)

    small_load = [
        pltpu.make_async_copy(source, target, local_sem.at[CHUNKS + 1 + n])
        for n, (source, target) in enumerate(
            (
                (cell_hbm, ints.at[0]),
                (live_hbm, ints.at[1]),
                (order_hbm, ints.at[2]),
                (value_hbm, floats.at[0]),
                (error_hbm, floats.at[1]),
                (src_hbm, src),
                (owners_hbm, owners),
            )
        )
    ]
    for copy in small_load:
        copy.start()
    w_load = pltpu.make_async_copy(weights, wv, local_sem.at[CHUNKS])
    w_load.start()

    for copy in small_load:
        copy.wait()
    lane = lax.broadcasted_iota(jnp.int32, (OBS, OBS), 0)
    perm = jnp.where(lane == ints[2], 1.0, 0.0)
    rows = [
        ints[0].astype(jnp.float32),
        floats[0],
        floats[1],
        ints[1].astype(jnp.float32),
    ]
    stacked = jnp.concatenate(rows + [jnp.zeros((4, OBS), jnp.float32)], axis=0)
    ordered = jnp.dot(
        stacked,
        perm,
        precision=lax.Precision.HIGHEST,
        preferred_element_type=jnp.float32,
    )
    meta_in[4] = jnp.concatenate([ordered, jnp.zeros((8, CELLS - OBS), jnp.float32)], axis=1)

    @pl.when(jnp.logical_not(has_far))
    def _():
        meta_in[slot(0, far)] = jnp.zeros((8, CELLS), jnp.float32)


    positions = [
        (src[0, k] // ny - i + 1) * 3 + (src[0, k] % ny - j + 1) for k in range(K)
    ]

    def product(dx, dy, c):
        p = slot(dx, dy)
        which = jnp.int32(0)
        valid = positions[0] == p
        for k in range(1, K):
            which = jnp.where(positions[k] == p, k, which)
            valid = jnp.logical_or(valid, positions[k] == p)
        part = jnp.dot(
            oce[home(dx, dy), c],
            wv[which, pl.ds(c * CW, CW), :],
            preferred_element_type=jnp.float32,
        )
        return jnp.where(valid, part, 0.0)

    w_load.wait()
    total = product(0, 0, 0)
    for c in range(1, CHUNKS):
        total = total + product(0, 0, c)
    acc[...] = total

    def add(dx, dy, piece):
        for c in range(piece[0], piece[0] + piece[1]):
            acc[...] += product(dx, dy, c)

    def from_y(piece, with_away):
        def one(dy, is_far):
            arrived(piece, 0, dy)
            send(is_far, False, piece, 0, dy, mate, 0)

        one(near, False)
        when_far(lambda: one(far, True))
        if with_away:

            @when_away
            def _():
                when_far(lambda: both_copy(piece, away, piece[0]).start())
                when_no_far(lambda: send(None, True, piece, 0, near, away, 0))

    from_y(FIRST, True)
    meta_copy(0, near, 0).start()
    when_far(lambda: meta_copy(0, far, 1).start())

    @when_away
    def _():
        arrived(THIRD, away, 0)
        send(False, True, THIRD, away, 0, 0, near)
        when_far(lambda: send(True, True, THIRD, away, 0, 0, far))

    from_y(SECOND, True)
    arrived(WHOLE, mate, 0)
    add(mate, 0, WHOLE)
    add(0, near, BOTH)
    when_far(lambda: add(0, far, BOTH))
    when_away(lambda: add(away, 0, THIRD))
    from_y(THIRD, False)
    add(0, near, THIRD)
    when_far(lambda: add(0, far, THIRD))

    meta_copy(0, -near, 0).wait_recv()
    when_far(lambda: meta_copy(0, -far, 1).wait_recv())
    meta_copy(mate, 0, 2).start()
    when_away(lambda: meta_copy(away, 0, 3).start())

    @when_away
    def _():
        arrived(BOTH, away, 0)
        add(away, 0, BOTH)

    def corner(dx, dy, piece):
        arrived(piece, dx, dy)
        add(dx, dy, piece)

    for piece in (FIRST, SECOND, THIRD):
        corner(mate, near, piece)
        when_far(lambda: corner(mate, far, piece))

    @when_away
    def _():
        for piece in (FIRST, SECOND):

            @when_far
            def _():
                both_copy(piece, -away, piece[0]).wait_recv()
                add(away, near, piece)
                add(away, far, piece)

            when_no_far(lambda: corner(away, near, piece))

        corner(away, near, THIRD)
        when_far(lambda: corner(away, far, THIRD))

    sst = acc[...]
    mean = jnp.sum(sst, axis=0, keepdims=True) / MEM
    anomaly = sst - mean
    pieces = [anomaly[8 * g : 8 * g + 8] for g in range(MEM // 8)]
    pieces.append(jnp.broadcast_to(mean, (8, CELLS)))
    lane8 = lax.broadcasted_iota(jnp.int32, (8, CELLS), 1)
    pair = (lane8 % AY) // 2
    quarter = lane8 // 32

    for block in range(2):
        west = jnp.zeros((8, CELLS), jnp.float32)
        east = west
        for g in range(8 * block, min(8 * block + 8, GROUPS)):
            s = g % 8
            moved = roll(pieces[g], 2 * s)
            west = jnp.where(pair == s, moved, west)
            east = jnp.where(pair == (s + 7) % 8, moved, east)
        pack_y[0, 8 * block : 8 * block + 8, :] = west
        pack_y[1, 8 * block : 8 * block + 8, :] = east
    for block in range(3):
        north = jnp.zeros((8, CELLS), jnp.float32)
        south = north
        for g in range(4 * block, min(4 * block + 4, GROUPS)):
            s = g % 4
            moved = roll(pieces[g], 32 * s)
            north = jnp.where(quarter == s, moved, north)
            south = jnp.where(quarter == (s + 3) % 4, moved, south)
        pack_x[0, 8 * block : 8 * block + 8, :] = north
        pack_x[1, 8 * block : 8 * block + 8, :] = south

    def halo_y(dx, dy):
        side = (dy + 1) // 2
        return pltpu.make_async_remote_copy(
            src_ref=pack_y.at[side],
            dst_ref=in_y.at[side, 1 - dx],
            send_sem=halo_send.at[slot(dx, dy)],
            recv_sem=halo_recv.at[slot(-dx, -dy)],
            device_id=device(dx, dy),
            device_id_type=MESH,
        )

    def halo_x(dx):
        side = (dx + 1) // 2
        return pltpu.make_async_remote_copy(
            src_ref=pack_x.at[side],
            dst_ref=in_x.at[side],
            send_sem=halo_send.at[slot(dx, 0)],
            recv_sem=halo_recv.at[slot(-dx, 0)],
            device_id=device(dx, 0),
            device_id_type=MESH,
        )

    @when_away
    def _():
        when_far(lambda: halo_y(away, far).start())
        halo_y(away, near).start()

    @when_far
    def _():
        halo_y(mate, far).start()
        halo_y(0, far).start()

    halo_y(mate, near).start()
    halo_y(0, near).start()
    when_away(lambda: halo_x(away).start())
    halo_x(mate).start()

    f_out[0, :MEM, :] = anomaly
    f_out[0, MEM:, :] = pieces[-1]
    for dx, dy in AROUND:
        for g in range(MEM // 8):
            own_shifts[slot(dx, dy), 8 * g : 8 * g + 8, :] = roll(pieces[g], -(AY * dx + dy))

    absent = jnp.where(lax.broadcasted_iota(jnp.int32, (8, CELLS), 0) == 2, 1.0, 0.0)
    meta_copy(-mate, 0, 2).wait_recv()
    when_away(lambda: meta_copy(-away, 0, 3).wait_recv())

    blocks = []
    for dx, dy in NEAR:
        if (dx, dy) == (0, 0):
            blocks.append(meta_in[4])
        else:
            blocks.append(jnp.where(has(dx, dy), meta_in[slot(dx, dy)], absent))
    blocks.append(jnp.zeros((CELLS - 72, CELLS), jnp.float32))
    columns[...] = jnp.concatenate(blocks, axis=0).T

    lane32 = lax.broadcasted_iota(jnp.int32, (OB, CELLS), 1)
    for batch in range(NB):
        rows = slice(batch * OB, (batch + 1) * OB)

        def dense(dx, dy, lanes):
            at = 8 * slot(dx, dy)
            cells, values, errors, alive = (
                jnp.broadcast_to(columns[rows, at + n : at + n + 1], (OB, CELLS))
                for n in range(4)
            )
            hit = jnp.where(cells == lanes, alive, 0.0)
            return hit, hit * values, errors + (1.0 - alive), errors

        cell_row = jnp.broadcast_to(owners[2 * batch : 2 * batch + 1, :], (OB, CELLS))
        tile_row = jnp.broadcast_to(owners[2 * batch + 1 : 2 * batch + 2, :], (OB, CELLS))
        cell_row = cell_row.astype(jnp.float32)
        around = dense(-1, -1, cell_row)
        for dx, dy in AROUND[1:]:
            other = dense(dx, dy, cell_row)
            chosen = tile_row == slot(dx, dy)
            around = tuple(jnp.where(chosen, n, o) for n, o in zip(other, around))
        for place, parts in enumerate((dense(0, 0, lane32.astype(jnp.float32)), around)):
            for n, part in enumerate(parts):
                obs_out[batch, place, n] = part

    def finish(far_needed, away_needed):
        for f, a, spec in sends:
            if (f, a) == (far_needed, away_needed):
                ocean_copy(*spec).wait_send()

    finish(False, False)
    meta_copy(0, near, 0).wait_send()
    meta_copy(mate, 0, 2).wait_send()

    @when_far
    def _():
        finish(True, False)
        meta_copy(0, far, 1).wait_send()

    @when_away
    def _():
        finish(False, True)
        meta_copy(away, 0, 3).wait_send()
        when_no_far(lambda: finish(None, True))

        @when_far
        def _():
            finish(True, True)
            for piece in (FIRST, SECOND):
                both_copy(piece, away, piece[0]).wait_send()

    halo_x(-mate).wait_recv()
    halo_y(0, -near).wait_recv()
    halo_y(-mate, -near).wait_recv()

    @when_far
    def _():
        halo_y(0, -far).wait_recv()
        halo_y(-mate, -far).wait_recv()

    @when_away
    def _():
        halo_x(-away).wait_recv()
        halo_y(-away, -near).wait_recv()
        when_far(lambda: halo_y(-away, -far).wait_recv())

    def present(ref, dx, dy):
        return jnp.where(has(dx, dy), ref[...], 0.0)

    north = present(in_x.at[0], 1, 0)
    south = present(in_x.at[1], -1, 0)
    west = present(in_y.at[0, 1], 0, 1)
    east = present(in_y.at[1, 1], 0, -1)
    corners = (
        present(in_y.at[0, 2], 1, 1),
        present(in_y.at[0, 0], -1, 1),
        present(in_y.at[1, 2], 1, -1),
        present(in_y.at[1, 0], -1, -1),
    )
    y8 = lane8 % AY
    beside = jnp.logical_or(y8 < 2, y8 >= AY - 2)
    for g in range(GROUPS):
        at = pl.ds(8 * g, 8)
        b, s = slice(8 * (g // 4), 8 * (g // 4) + 8), g % 4
        f_out[1, at, :] = roll(jnp.where(quarter == s, north[b], south[b]), -32 * s)
        b, s = slice(8 * (g // 8), 8 * (g // 8) + 8), g % 8
        from_west = pair == s
        sides = roll(jnp.where(from_west, west[b], east[b]), -2 * s)
        low_x = jnp.logical_and(lane8 >= 2 * s, lane8 < 64 + 2 * s)
        corner = jnp.where(
            from_west,
            jnp.where(low_x, corners[0][b], corners[1][b]),
            jnp.where(low_x, corners[2][b], corners[3][b]),
        )
        f_out[2, at, :] = jnp.where(beside, sides, roll(corner, 4 - 2 * s))

    halo_x(mate).wait_send()
    halo_y(0, near).wait_send()
    halo_y(mate, near).wait_send()

    @when_far
    def _():
        halo_y(0, far).wait_send()
        halo_y(mate, far).wait_send()

    @when_away
    def _():
        halo_x(away).wait_send()
        halo_y(away, near).wait_send()
        when_far(lambda: halo_y(away, far).wait_send())


def update_kernel(
    f_in,
    own_shifts,
    obs,
    tables,
    atm,
    mean_out,
    anom_out,
    around,
    state,
    first_shifts,
    other_shifts,
    second_shifts,
    factors,
    covariance,
    result,
    field_mean,
    means,
    out_sem,
    mean_sem,
):
    lane8 = lax.broadcasted_iota(jnp.int32, (8, CELLS), 1)
    groups = range(MEM // 8)
    pairs = FIELDS // 2

    def region(n):
        return pl.when(lax.axis_index("gx") > -1 - n)


    def at(g):
        return slice(8 * g, 8 * g + 8)

    def take(block, lanes):
        return jnp.take_along_axis(block, lanes, axis=1, mode="promise_in_bounds")

    def shift(base, d, own, ring):
        if d == 4 and base != 9:
            return own
        table = tables[base + d]
        lanes = jnp.bitwise_and(table, CELLS - 1)
        if d == 4:
            return take(ring, lanes)
        return jnp.where(table >= CELLS, take(ring, lanes), take(own, lanes))

    def allsum(x):
        for step in (4, 2, 1):
            x = x + pltpu.roll(x, step, 0)
        return x

    zero = jnp.zeros((8, CELLS), jnp.float32)
    tapers = [
        max(1.0 - (dx * dx + dy * dy) / 4.0, 0.0) ** 2 / (MEM - 1) for dx, dy in NEAR
    ]

    def observe(batch, sources, bases):
        alphas, betas = [], []
        for f, source in enumerate(sources):
            square = zero
            for g in groups:
                block = source[at(g), :]
                square = square + block * block
            variance = allsum(square) / (MEM - 1)
            total = [zero, zero, zero]
            for q in range(OB // 8):
                masked = obs[batch, f, 0, at(q), :]
                masked_value = obs[batch, f, 1, at(q), :]
                inverse = 1.0 / (variance + obs[batch, f, 2, at(q), :])
                ratio = obs[batch, f, 3, at(q), :] * inverse
                damping = 1.0 / (1.0 + ratio * lax.rsqrt(ratio))
                weighting = masked * inverse
                total[0] = total[0] + weighting * damping
                total[1] = total[1] + weighting
                total[2] = total[2] + masked_value * inverse
            betas.append(allsum(total[0]))
            alphas.append(allsum(total[2]) - source[MEM:, :] * allsum(total[1]))
        for base in bases:
            for kind, blocks in enumerate((alphas, betas)):
                for d in range(9):
                    factors[kind, base + d] = shift(base, d, *blocks) * tapers[d]

    def shift_groups(base, target, own, ring, chosen):
        for g in chosen:
            for d in range(9):
                target[d, at(g), :] = shift(base, d, own[at(g), :], ring[at(g), :])

    def sst_step(base, source, mean, shifts, store):
        sums = [zero] * 9
        for g in groups:
            block = source[at(g), :]
            for d in range(9):
                sums[d] = sums[d] + shifts[d, at(g), :] * block
        sums = [allsum(x) for x in sums]
        for d in range(9):
            mean = mean + factors[0, base + d] * sums[d]
        gains = [factors[1, base + d] * sums[d] for d in range(9)]
        for g in groups:
            block = source[at(g), :]
            for d in range(9):
                block = block - shifts[d, at(g), :] * gains[d]
            store[at(g), :] = block
        return mean

    def field_step(base, shifted, fields, sums):
        mean = [field_mean[u] for u in fields]
        for n, u in enumerate(fields):
            for d in range(9):
                mean[n] = mean[n] + factors[0, base + d] * sums[n][d]
        gains = [[factors[1, base + d] * sums[n][d] for d in range(9)] for n in range(2)]
        for g in groups:
            for n, u in enumerate(fields):
                block = result[u, at(g), :]
                for d in range(9):
                    block = block - shifted[d, at(g), :] * gains[n][d]
                result[u, at(g), :] = block
        return mean

    gathered = tables[27]
    edge = jnp.logical_or(lane8 < 32, lane8 >= 96)
    for g in range(GROUPS):
        around[at(g), :] = jnp.where(edge, f_in[1, at(g), :], take(f_in[2, at(g), :], gathered))
    own = f_in.at[0]
    for g in groups:
        first_shifts[4, at(g), :] = own[at(g), :]
        for d in range(9):
            if d != 4:
                lanes = jnp.bitwise_and(tables[d], CELLS - 1)
                first_shifts[d, at(g), :] = jnp.where(
                    tables[d] >= CELLS, take(around[at(g), :], lanes), own_shifts[d, at(g), :]
                )
    observe(0, (own, around), (0, 9))

    for u in range(FIELDS):
        total = zero
        for g in groups:
            total = total + atm[u, at(g), :]
        mean = allsum(total) / MEM
        field_mean[u] = mean
        for g in groups:
            result[u, at(g), :] = atm[u, at(g), :] - mean


    def reduce_covariance(pair):
        for u in (2 * pair, 2 * pair + 1):
            for d in range(9):
                covariance[u, d] = allsum(covariance[u, d])

    def first_covariance(pair):
        fields = (2 * pair, 2 * pair + 1)
        if pair > 0:
            reduce_covariance(pair - 1)
        sums = [[zero] * 9, [zero] * 9]
        for g in groups:
            for n, u in enumerate(fields):
                block = result[u, at(g), :]
                for d in range(9):
                    sums[n][d] = sums[n][d] + first_shifts[d, at(g), :] * block
        for n, u in enumerate(fields):
            for d in range(9):
                covariance[u, d] = sums[n][d]
        shift_groups(9, other_shifts, own, around, groups[2 * pair : 2 * pair + 2])

    for pair in range(pairs):
        region(pair)(functools.partial(first_covariance, pair))
    reduce_covariance(pairs - 1)
    state[0, MEM:, :] = sst_step(0, own, own[MEM:, :], first_shifts, state.at[0])
    mean = shift(9, 4, own[MEM:, :], around[MEM:, :])
    state[1, MEM:, :] = sst_step(9, other_shifts.at[4], mean, other_shifts, state.at[1])
    observe(1, (state.at[0], state.at[1]), (18,))

    def first_update(pair):
        fields = (2 * pair, 2 * pair + 1)
        sums = [[covariance[u, d] for d in range(9)] for u in fields]
        mean = field_step(0, first_shifts, fields, sums)
        for n, u in enumerate(fields):
            field_mean[u] = mean[n]
        shift_groups(
            18, second_shifts, state.at[0], state.at[1], groups[2 * pair : 2 * pair + 2]
        )

    for pair in range(pairs):
        region(pairs + pair)(functools.partial(first_update, pair))
    mean = sst_step(18, state.at[0], state[0, MEM:, :], second_shifts, result.at[FIELDS])
    means[FIELDS] = mean[:1]
    sst_copy = pltpu.make_async_copy(result.at[FIELDS], anom_out.at[FIELDS], mean_sem.at[1])
    sst_copy.start()

    def field_copy(pair):
        part = pl.ds(2 * pair, 2)
        return pltpu.make_async_copy(result.at[part], anom_out.at[part], out_sem.at[pair])

    def second_batch(pair):
        fields = (2 * pair, 2 * pair + 1)
        sums = [[zero] * 9, [zero] * 9]
        for g in groups:
            for n, u in enumerate(fields):
                block = result[u, at(g), :]
                for d in range(9):
                    sums[n][d] = sums[n][d] + second_shifts[d, at(g), :] * block
        sums = [[allsum(x) for x in sums[n]] for n in range(2)]
        mean = field_step(18, second_shifts, fields, sums)
        for n, u in enumerate(fields):
            means[u] = mean[n][:1]
        field_copy(pair).start()

    for pair in range(pairs):
        region(2 * pairs + pair)(functools.partial(second_batch, pair))
    mean_copy = pltpu.make_async_copy(means, mean_out, mean_sem.at[0])
    mean_copy.start()
    sst_copy.wait()
    for pair in range(pairs):
        field_copy(pair).wait()
    mean_copy.wait()


def local(
    atm_members,
    ocean_members,
    remap_weights,
    pair_src,
    obs_cell,
    obs_value,
    obs_error,
    obs_live,
    obs_order,
):
    f32 = jnp.float32
    shifts, owners = build_tables()
    vmem = pl.BlockSpec(memory_space=pltpu.VMEM)
    hbm = pl.BlockSpec(memory_space=pltpu.HBM)
    dma = pltpu.SemaphoreType.DMA
    state, own_shifts, tables = pl.pallas_call(
        exchange_kernel,
        out_shape=(
            jax.ShapeDtypeStruct((3, ROWS, CELLS), f32),
            jax.ShapeDtypeStruct((9, MEM, CELLS), f32),
            jax.ShapeDtypeStruct((NB, 2, 4, OB, CELLS), f32),
        ),
        in_specs=[hbm] * 9,
        out_specs=(vmem, vmem, vmem),
        scratch_shapes=[
            pltpu.SMEM((1, K), jnp.int32),
            pltpu.VMEM((8, CELLS), jnp.int32),
            pltpu.VMEM((3, 1, OBS), jnp.int32),
            pltpu.VMEM((2, 1, OBS), f32),
            pltpu.VMEM((9, CHUNKS, MEM, CW), jnp.bfloat16),
            pltpu.VMEM((K, OCN_DEV, CELLS), jnp.bfloat16),
            pltpu.VMEM((MEM, CELLS), f32),
            pltpu.VMEM((CELLS, CELLS), f32),
            pltpu.VMEM((9, 8, CELLS), f32),
            pltpu.VMEM((2, 16, CELLS), f32),
            pltpu.VMEM((2, 24, CELLS), f32),
            pltpu.VMEM((2, 3, 16, CELLS), f32),
            pltpu.VMEM((2, 24, CELLS), f32),
            dma((CHUNKS + 8,)),
            dma((24,)),
            dma((9, CHUNKS)),
            dma((2,)),
            dma((2,)),
            dma((4,)),
            dma((9,)),
            dma((9,)),
            dma((9,)),
        ],
        compiler_params=pltpu.CompilerParams(
            collective_id=0, has_side_effects=True, vmem_limit_bytes=16 * 1024 * 1024
        ),
    )(
        *(
            pltpu.with_memory_space_constraint(x, pltpu.HBM)
            for x in (
                pair_src[0],
                ocean_members[0, 0],
                remap_weights[0, 0],
                obs_cell[0],
                obs_value[0],
                obs_error[0],
                obs_live[0],
                obs_order[0],
                jnp.asarray(owners),
            )
        )
    )
    mean, anomaly = pl.pallas_call(
        update_kernel,
        out_shape=(
            jax.ShapeDtypeStruct((COMP, 1, CELLS), f32),
            jax.ShapeDtypeStruct((COMP, MEM, CELLS), f32),
        ),
        in_specs=[vmem] * 5,
        out_specs=(hbm, hbm),
        scratch_shapes=[
            pltpu.VMEM((ROWS, CELLS), f32),
            pltpu.VMEM((2, ROWS, CELLS), f32),
            pltpu.VMEM((9, MEM, CELLS), f32),
            pltpu.VMEM((9, MEM, CELLS), f32),
            pltpu.VMEM((9, MEM, CELLS), f32),
            pltpu.VMEM((2, 27, 8, CELLS), f32),
            pltpu.VMEM((FIELDS, 9, 8, CELLS), f32),
            pltpu.VMEM((COMP, MEM, CELLS), f32),
            pltpu.VMEM((FIELDS, 8, CELLS), f32),
            pltpu.VMEM((COMP, 1, CELLS), f32),
            dma((FIELDS // 2,)),
            dma((2,)),
        ],
        compiler_params=pltpu.CompilerParams(vmem_limit_bytes=16 * 1024 * 1024),
    )(state, own_shifts, tables, jnp.asarray(shifts), jnp.transpose(atm_members[0, 0], (1, 0, 2)))
    return (mean.reshape(1, 1, COMP, CELLS), jnp.transpose(anomaly, (1, 0, 2))[None, None])


def solution(mesh):
    in_specs = (
        P("gx", "gy", None, None, None),
        P("gx", "gy", None, None),
        P("gx", "gy", None, None, None),
        P("gx", "gy", None),
        P("gx", "gy", None),
        P("gx", "gy", None),
        P("gx", "gy", None),
        P("gx", "gy", None),
        P("gx", "gy", None),
    )
    out_specs = (P("gx", "gy", None, None), P("gx", "gy", None, None, None))
    return jax.shard_map(local, mesh=mesh, in_specs=in_specs, out_specs=out_specs, check_vma=False)
```

```python
import functools

import jax
import jax.numpy as jnp
import numpy as np
from jax import lax
from jax.experimental import pallas as pl
from jax.experimental.pallas import tpu as pltpu
from jax.sharding import PartitionSpec as P

MEM = 80
AX = 8
AY = 16
OCN_DEV = 1024
OB = 32
NB = 2
K = 4
FIELDS = 12
COMP = 13
CELLS = 128
OBS = 64
ROWS = 88
GROUPS = 11
CHUNKS = 4
CW = OCN_DEV // CHUNKS
FIRST, SECOND, THIRD, BOTH, WHOLE = (0, 1), (1, 1), (2, 2), (0, 2), (0, 4)

MESH = pl.DeviceIdType.MESH
NEAR = [(dx, dy) for dx in (-1, 0, 1) for dy in (-1, 0, 1)]
AROUND = [d for d in NEAR if d != (0, 0)]


def build_tables():
    ring_e, ring_r, gathered = {}, {}, np.zeros(CELLS, np.int32)
    middle = {0: 32, 1: 64}
    for x in range(-2, AX + 2):
        for y in range(-2, AY + 2):
            out_x, out_y = not 0 <= x < AX, not 0 <= y < AY
            if not (out_x or out_y):
                continue
            lane = (x % AX) * AY + y % AY
            if out_y:
                gathered[middle[out_x]] = (lane + 4 * out_x) % CELLS
                lane = middle[out_x]
                middle[out_x] += 1
            ring_e[x, y] = lane
            if -1 <= x <= AX and -1 <= y <= AY:
                ring_r[x, y] = len(ring_r)

    def code(x, y, ring):
        inside = 0 <= x < AX and 0 <= y < AY
        return x * AY + y if inside else CELLS + ring[x, y]

    shifts = np.zeros((28, CELLS), np.int32)
    for d, (dx, dy) in enumerate(NEAR):
        for c in range(CELLS):
            x, y = c // AY + dx, c % AY + dy
            shifts[d, c] = code(x, y, ring_e)
            shifts[18 + d, c] = code(x, y, ring_r)
        for (x, y), lane in ring_r.items():
            shifts[9 + d, lane] = code(x + dx, y + dy, ring_e)
    shifts[27] = gathered
    owners = np.full((8, CELLS), -1, np.int32)
    for n, ring in enumerate((ring_e, ring_r)):
        for (x, y), lane in ring.items():
            owners[2 * n, lane] = (x % AX) * AY + y % AY
            owners[2 * n + 1, lane] = slot(x // AX, y // AY)
    return np.repeat(shifts[:, None], 8, axis=1), owners


def slot(dx, dy):
    return (dx + 1) * 3 + dy + 1


def home(dx, dy):
    return (dx + 1) * 3 + (2 if isinstance(dy, int) and dy == 0 else (dy + 1) // 2)


def roll(x, shift):
    shift = shift % CELLS
    return x if shift == 0 else pltpu.roll(x, shift, 1)


def exchange_kernel(
    src_hbm,
    ocean,
    weights,
    cell_hbm,
    value_hbm,
    error_hbm,
    live_hbm,
    order_hbm,
    owners_hbm,
    f_out,
    own_shifts,
    obs_out,
    src,
    owners,
    ints,
    floats,
    oce,
    wv,
    acc,
    columns,
    meta_in,
    pack_y,
    pack_x,
    in_y,
    in_x,
    local_sem,
    oce_send,
    oce_recv,
    both_send,
    both_recv,
    meta_send,
    meta_recv,
    halo_send,
    halo_recv,
):
    i = lax.axis_index("gx")
    j = lax.axis_index("gy")
    nx = lax.axis_size("gx")
    ny = lax.axis_size("gy")

    away = 2 * (i % 2) - 1
    mate = -away
    has_away = jnp.logical_and(i + away >= 0, i + away < nx)
    near = 1 - 2 * ((j % 4 + 3) // 4)
    far = -near
    has_far = jnp.logical_and(j + far >= 0, j + far < ny)
    when_away, when_far = pl.when(has_away), pl.when(has_far)
    when_no_far = pl.when(jnp.logical_not(has_far))

    def has(dx, dy):
        cond = None
        for pos, step, count in ((i, dx, nx), (j, dy, ny)):
            if step:
                ok = (pos > 0) if step < 0 else (pos < count - 1)
                cond = ok if cond is None else jnp.logical_and(cond, ok)
        return cond

    def when(dx, dy):
        return pl.when(has(dx, dy))

    def device(dx, dy):
        return (i + dx, j + dy)

    own_load = [
        pltpu.make_async_copy(
            ocean.at[:, pl.ds(c * CW, CW)], oce.at[home(0, 0), c], local_sem.at[c]
        )
        for c in range(CHUNKS)
    ]
    for copy in own_load:
        copy.start()

    barrier = pltpu.get_barrier_semaphore()

    def greet(dx, dy):
        pl.semaphore_signal(barrier, inc=1, device_id=device(dx, dy), device_id_type=MESH)

    @when_far
    def _():
        greet(0, far)

    greet(0, near)

    @when_away
    def _():
        greet(away, 0)

    greet(mate, 0)

    pl.semaphore_wait(
        barrier,
        2 + has_away.astype(jnp.int32) + has_far.astype(jnp.int32),
    )

    def tile(p, piece):
        return oce.at[p, pl.ds(*piece)]

    def ocean_copy(piece, from_dx, from_dy, dx, dy, sem):
        target = home(from_dx - dx, from_dy - dy)
        return pltpu.make_async_remote_copy(
            src_ref=tile(home(from_dx, from_dy), piece),
            dst_ref=tile(target, piece),
            send_sem=oce_send.at[sem],
            recv_sem=oce_recv.at[target, piece[0]],
            device_id=device(dx, dy),
            device_id_type=MESH,
        )

    def arrived(piece, dx, dy):
        ocean_copy(piece, 0, 0, -dx, -dy, 0).wait_recv()

    def both_copy(piece, dx, sem):
        target = home(-dx, -1)
        return pltpu.make_async_remote_copy(
            src_ref=oce.at[pl.ds(home(0, -1), 2), pl.ds(*piece)],
            dst_ref=oce.at[pl.ds(target, 2), pl.ds(*piece)],
            send_sem=both_send.at[sem],
            recv_sem=both_recv.at[sem],
            device_id=device(dx, 0),
            device_id_type=MESH,
        )

    def meta_copy(dx, dy, sem):
        if isinstance(dx, int):
            source, target = meta_in.at[4], meta_in.at[slot(0, -dy)]
            recv = meta_recv.at[slot(0, -dy)]
        else:
            source, target = meta_in.at[pl.ds(3, 3)], meta_in.at[pl.ds(slot(-dx, -1), 3)]
            recv = meta_recv.at[slot(-dx, 0)]
        return pltpu.make_async_remote_copy(
            src_ref=source,
            dst_ref=target,
            send_sem=meta_send.at[sem],
            recv_sem=recv,
            device_id=device(dx, dy),
            device_id_type=MESH,
        )

    sends = []

    def send(far_needed, away_needed, *spec):
        sends.append((far_needed, away_needed, spec + (len(sends),)))
        ocean_copy(*sends[-1][2]).start()

    for c in range(CHUNKS):
        own_load[c].wait()
        if c == 0:
            send(False, False, FIRST, 0, 0, 0, near)
            when_far(lambda: send(True, False, FIRST, 0, 0, 0, far))
        if c == 1:
            send(False, False, SECOND, 0, 0, 0, near)
            when_far(lambda: send(True, False, SECOND, 0, 0, 0, far))
        if c == 3:

            @when_away
            def _():
                send(False, True, THIRD, 0, 0, away, 0)
                send(False, True, BOTH, 0, 0, away, 0)

            send(False, False, THIRD, 0, 0, 0, near)
            when_far(lambda: send(True, False, THIRD, 0, 0, 0, far))
            send(False, False, WHOLE, 0, 0, mate, 0)

    small_load = [
        pltpu.make_async_copy(source, target, local_sem.at[CHUNKS + 1 + n])
        for n, (source, target) in enumerate(
            (
                (cell_hbm, ints.at[0]),
                (live_hbm, ints.at[1]),
                (order_hbm, ints.at[2]),
                (value_hbm, floats.at[0]),
                (error_hbm, floats.at[1]),
                (src_hbm, src),
                (owners_hbm, owners),
            )
        )
    ]
    for copy in small_load:
        copy.start()
    w_load = pltpu.make_async_copy(weights, wv, local_sem.at[CHUNKS])
    w_load.start()

    for copy in small_load:
        copy.wait()
    lane = lax.broadcasted_iota(jnp.int32, (OBS, OBS), 0)
    perm = jnp.where(lane == ints[2], 1.0, 0.0)
    rows = [
        ints[0].astype(jnp.float32),
        floats[0],
        floats[1],
        ints[1].astype(jnp.float32),
    ]
    stacked = jnp.concatenate(rows + [jnp.zeros((4, OBS), jnp.float32)], axis=0)
    ordered = jnp.dot(
        stacked,
        perm,
        precision=lax.Precision.HIGHEST,
        preferred_element_type=jnp.float32,
    )
    meta_in[4] = jnp.concatenate([ordered, jnp.zeros((8, CELLS - OBS), jnp.float32)], axis=1)

    @pl.when(jnp.logical_not(has_far))
    def _():
        meta_in[slot(0, far)] = jnp.zeros((8, CELLS), jnp.float32)


    positions = [
        (src[0, k] // ny - i + 1) * 3 + (src[0, k] % ny - j + 1) for k in range(K)
    ]

    def product(dx, dy, c):
        p = slot(dx, dy)
        which = jnp.int32(0)
        valid = positions[0] == p
        for k in range(1, K):
            which = jnp.where(positions[k] == p, k, which)
            valid = jnp.logical_or(valid, positions[k] == p)
        part = jnp.dot(
            oce[home(dx, dy), c],
            wv[which, pl.ds(c * CW, CW), :],
            preferred_element_type=jnp.float32,
        )
        return jnp.where(valid, part, 0.0)

    w_load.wait()
    total = product(0, 0, 0)
    for c in range(1, CHUNKS):
        total = total + product(0, 0, c)
    acc[...] = total

    def add(dx, dy, piece):
        for c in range(piece[0], piece[0] + piece[1]):
            acc[...] += product(dx, dy, c)

    def from_y(piece, with_away, between=lambda: None):
        def one(dy, is_far):
            arrived(piece, 0, dy)
            send(is_far, False, piece, 0, dy, mate, 0)

        one(near, False)
        between()
        when_far(lambda: one(far, True))
        if with_away:

            @when_away
            def _():
                when_far(lambda: both_copy(piece, away, piece[0]).start())
                when_no_far(lambda: send(None, True, piece, 0, near, away, 0))

    def from_away():
        arrived(THIRD, away, 0)
        send(False, True, THIRD, away, 0, 0, near)
        when_far(lambda: send(True, True, THIRD, away, 0, 0, far))

    from_y(FIRST, True, lambda: when_away(from_away))
    meta_copy(0, near, 0).start()
    when_far(lambda: meta_copy(0, far, 1).start())
    from_y(SECOND, True)
    arrived(WHOLE, mate, 0)
    add(mate, 0, WHOLE)
    add(0, near, BOTH)
    when_far(lambda: add(0, far, BOTH))
    when_away(lambda: add(away, 0, THIRD))
    from_y(THIRD, False)
    add(0, near, THIRD)
    when_far(lambda: add(0, far, THIRD))

    meta_copy(0, -near, 0).wait_recv()
    when_far(lambda: meta_copy(0, -far, 1).wait_recv())
    meta_copy(mate, 0, 2).start()
    when_away(lambda: meta_copy(away, 0, 3).start())

    @when_away
    def _():
        arrived(BOTH, away, 0)
        add(away, 0, BOTH)

    def corner(dx, dy, piece):
        arrived(piece, dx, dy)
        add(dx, dy, piece)

    for piece in (FIRST, SECOND, THIRD):
        corner(mate, near, piece)
        when_far(lambda: corner(mate, far, piece))

    @when_away
    def _():
        for piece in (FIRST, SECOND):

            @when_far
            def _():
                both_copy(piece, -away, piece[0]).wait_recv()
                add(away, near, piece)
                add(away, far, piece)

            when_no_far(lambda: corner(away, near, piece))

        corner(away, near, THIRD)
        when_far(lambda: corner(away, far, THIRD))

    sst = acc[...]
    mean = jnp.sum(sst, axis=0, keepdims=True) / MEM
    anomaly = sst - mean
    pieces = [anomaly[8 * g : 8 * g + 8] for g in range(MEM // 8)]
    pieces.append(jnp.broadcast_to(mean, (8, CELLS)))
    lane8 = lax.broadcasted_iota(jnp.int32, (8, CELLS), 1)
    pair = (lane8 % AY) // 2
    quarter = lane8 // 32

    for block in range(2):
        west = jnp.zeros((8, CELLS), jnp.float32)
        east = west
        for g in range(8 * block, min(8 * block + 8, GROUPS)):
            s = g % 8
            moved = roll(pieces[g], 2 * s)
            west = jnp.where(pair == s, moved, west)
            east = jnp.where(pair == (s + 7) % 8, moved, east)
        pack_y[0, 8 * block : 8 * block + 8, :] = west
        pack_y[1, 8 * block : 8 * block + 8, :] = east
    def halo_y(dx, dy):
        side = (dy + 1) // 2
        return pltpu.make_async_remote_copy(
            src_ref=pack_y.at[side],
            dst_ref=in_y.at[side, 1 - dx],
            send_sem=halo_send.at[slot(dx, dy)],
            recv_sem=halo_recv.at[slot(-dx, -dy)],
            device_id=device(dx, dy),
            device_id_type=MESH,
        )

    def halo_x(dx):
        side = (dx + 1) // 2
        return pltpu.make_async_remote_copy(
            src_ref=pack_x.at[side],
            dst_ref=in_x.at[side],
            send_sem=halo_send.at[slot(dx, 0)],
            recv_sem=halo_recv.at[slot(-dx, 0)],
            device_id=device(dx, 0),
            device_id_type=MESH,
        )

    @when_away
    def _():
        when_far(lambda: halo_y(away, far).start())
        halo_y(away, near).start()

    @when_far
    def _():
        halo_y(mate, far).start()
        halo_y(0, far).start()

    halo_y(mate, near).start()
    halo_y(0, near).start()
    for block in range(3):
        north = jnp.zeros((8, CELLS), jnp.float32)
        south = north
        for g in range(4 * block, min(4 * block + 4, GROUPS)):
            s = g % 4
            moved = roll(pieces[g], 32 * s)
            north = jnp.where(quarter == s, moved, north)
            south = jnp.where(quarter == (s + 3) % 4, moved, south)
        pack_x[0, 8 * block : 8 * block + 8, :] = north
        pack_x[1, 8 * block : 8 * block + 8, :] = south

    when_away(lambda: halo_x(away).start())
    halo_x(mate).start()

    f_out[0, :MEM, :] = anomaly
    f_out[0, MEM:, :] = pieces[-1]
    for dx, dy in AROUND:
        for g in range(MEM // 8):
            own_shifts[slot(dx, dy), 8 * g : 8 * g + 8, :] = roll(pieces[g], -(AY * dx + dy))

    absent = jnp.where(lax.broadcasted_iota(jnp.int32, (8, CELLS), 0) == 2, 1.0, 0.0)
    meta_copy(-mate, 0, 2).wait_recv()
    when_away(lambda: meta_copy(-away, 0, 3).wait_recv())

    blocks = []
    for dx, dy in NEAR:
        if (dx, dy) == (0, 0):
            blocks.append(meta_in[4])
        else:
            blocks.append(jnp.where(has(dx, dy), meta_in[slot(dx, dy)], absent))
    blocks.append(jnp.zeros((CELLS - 72, CELLS), jnp.float32))
    columns[...] = jnp.concatenate(blocks, axis=0).T

    lane32 = lax.broadcasted_iota(jnp.int32, (OB, CELLS), 1)
    for batch in range(NB):
        rows = slice(batch * OB, (batch + 1) * OB)

        def dense(dx, dy, lanes):
            at = 8 * slot(dx, dy)
            cells, values, errors, alive = (
                jnp.broadcast_to(columns[rows, at + n : at + n + 1], (OB, CELLS))
                for n in range(4)
            )
            hit = jnp.where(cells == lanes, alive, 0.0)
            return hit, hit * values, errors + (1.0 - alive), errors

        cell_row = jnp.broadcast_to(owners[2 * batch : 2 * batch + 1, :], (OB, CELLS))
        tile_row = jnp.broadcast_to(owners[2 * batch + 1 : 2 * batch + 2, :], (OB, CELLS))
        cell_row = cell_row.astype(jnp.float32)
        around = dense(-1, -1, cell_row)
        for dx, dy in AROUND[1:]:
            other = dense(dx, dy, cell_row)
            chosen = tile_row == slot(dx, dy)
            around = tuple(jnp.where(chosen, n, o) for n, o in zip(other, around))
        for place, parts in enumerate((dense(0, 0, lane32.astype(jnp.float32)), around)):
            for n, part in enumerate(parts):
                obs_out[batch, place, n] = part

    def finish(far_needed, away_needed):
        for f, a, spec in sends:
            if (f, a) == (far_needed, away_needed):
                ocean_copy(*spec).wait_send()

    finish(False, False)
    meta_copy(0, near, 0).wait_send()
    meta_copy(mate, 0, 2).wait_send()

    @when_far
    def _():
        finish(True, False)
        meta_copy(0, far, 1).wait_send()

    @when_away
    def _():
        finish(False, True)
        meta_copy(away, 0, 3).wait_send()
        when_no_far(lambda: finish(None, True))

        @when_far
        def _():
            finish(True, True)
            for piece in (FIRST, SECOND):
                both_copy(piece, away, piece[0]).wait_send()

    halo_x(-mate).wait_recv()
    halo_y(0, -near).wait_recv()
    halo_y(-mate, -near).wait_recv()

    @when_far
    def _():
        halo_y(0, -far).wait_recv()
        halo_y(-mate, -far).wait_recv()

    @when_away
    def _():
        halo_x(-away).wait_recv()
        halo_y(-away, -near).wait_recv()
        when_far(lambda: halo_y(-away, -far).wait_recv())

    def present(ref, dx, dy):
        return jnp.where(has(dx, dy), ref[...], 0.0)

    north = present(in_x.at[0], 1, 0)
    south = present(in_x.at[1], -1, 0)
    west = present(in_y.at[0, 1], 0, 1)
    east = present(in_y.at[1, 1], 0, -1)
    corners = (
        present(in_y.at[0, 2], 1, 1),
        present(in_y.at[0, 0], -1, 1),
        present(in_y.at[1, 2], 1, -1),
        present(in_y.at[1, 0], -1, -1),
    )
    y8 = lane8 % AY
    beside = jnp.logical_or(y8 < 2, y8 >= AY - 2)
    for g in range(GROUPS):
        at = pl.ds(8 * g, 8)
        b, s = slice(8 * (g // 4), 8 * (g // 4) + 8), g % 4
        f_out[1, at, :] = roll(jnp.where(quarter == s, north[b], south[b]), -32 * s)
        b, s = slice(8 * (g // 8), 8 * (g // 8) + 8), g % 8
        from_west = pair == s
        sides = roll(jnp.where(from_west, west[b], east[b]), -2 * s)
        low_x = jnp.logical_and(lane8 >= 2 * s, lane8 < 64 + 2 * s)
        corner = jnp.where(
            from_west,
            jnp.where(low_x, corners[0][b], corners[1][b]),
            jnp.where(low_x, corners[2][b], corners[3][b]),
        )
        f_out[2, at, :] = jnp.where(beside, sides, roll(corner, 4 - 2 * s))

    halo_x(mate).wait_send()
    halo_y(0, near).wait_send()
    halo_y(mate, near).wait_send()

    @when_far
    def _():
        halo_y(0, far).wait_send()
        halo_y(mate, far).wait_send()

    @when_away
    def _():
        halo_x(away).wait_send()
        halo_y(away, near).wait_send()
        when_far(lambda: halo_y(away, far).wait_send())


def update_kernel(
    f_in,
    own_shifts,
    obs,
    tables,
    atm,
    mean_out,
    anom_out,
    around,
    state,
    first_shifts,
    other_shifts,
    second_shifts,
    factors,
    covariance,
    result,
    field_mean,
    means,
    out_sem,
    mean_sem,
):
    lane8 = lax.broadcasted_iota(jnp.int32, (8, CELLS), 1)
    groups = range(MEM // 8)
    pairs = FIELDS // 2

    def region(n):
        return pl.when(lax.axis_index("gx") > -1 - n)


    def at(g):
        return slice(8 * g, 8 * g + 8)

    def take(block, lanes):
        return jnp.take_along_axis(block, lanes, axis=1, mode="promise_in_bounds")

    def shift(base, d, own, ring):
        if d == 4 and base != 9:
            return own
        table = tables[base + d]
        lanes = jnp.bitwise_and(table, CELLS - 1)
        if d == 4:
            return take(ring, lanes)
        return jnp.where(table >= CELLS, take(ring, lanes), take(own, lanes))

    def allsum(x):
        for step in (4, 2, 1):
            x = x + pltpu.roll(x, step, 0)
        return x

    zero = jnp.zeros((8, CELLS), jnp.float32)
    tapers = [
        max(1.0 - (dx * dx + dy * dy) / 4.0, 0.0) ** 2 / (MEM - 1) for dx, dy in NEAR
    ]

    def observe(batch, sources, bases):
        alphas, betas = [], []
        for f, source in enumerate(sources):
            square = zero
            for g in groups:
                block = source[at(g), :]
                square = square + block * block
            variance = allsum(square) / (MEM - 1)
            total = [zero, zero, zero]
            for q in range(OB // 8):
                masked = obs[batch, f, 0, at(q), :]
                masked_value = obs[batch, f, 1, at(q), :]
                inverse = 1.0 / (variance + obs[batch, f, 2, at(q), :])
                ratio = obs[batch, f, 3, at(q), :] * inverse
                damping = 1.0 / (1.0 + ratio * lax.rsqrt(ratio))
                weighting = masked * inverse
                total[0] = total[0] + weighting * damping
                total[1] = total[1] + weighting
                total[2] = total[2] + masked_value * inverse
            betas.append(allsum(total[0]))
            alphas.append(allsum(total[2]) - source[MEM:, :] * allsum(total[1]))
        for base in bases:
            for kind, blocks in enumerate((alphas, betas)):
                for d in range(9):
                    factors[kind, base + d] = shift(base, d, *blocks) * tapers[d]

    def shift_groups(base, target, own, ring, chosen):
        for g in chosen:
            for d in range(9):
                target[d, at(g), :] = shift(base, d, own[at(g), :], ring[at(g), :])

    def sst_step(base, source, mean, shifts, store):
        sums = [zero] * 9
        for g in groups:
            block = source[at(g), :]
            for d in range(9):
                sums[d] = sums[d] + shifts[d, at(g), :] * block
        sums = [allsum(x) for x in sums]
        for d in range(9):
            mean = mean + factors[0, base + d] * sums[d]
        gains = [factors[1, base + d] * sums[d] for d in range(9)]
        for g in groups:
            block = source[at(g), :]
            for d in range(9):
                block = block - shifts[d, at(g), :] * gains[d]
            store[at(g), :] = block
        return mean

    def field_step(base, shifted, fields, sums):
        mean = [field_mean[u] for u in fields]
        for n, u in enumerate(fields):
            for d in range(9):
                mean[n] = mean[n] + factors[0, base + d] * sums[n][d]
        gains = [[factors[1, base + d] * sums[n][d] for d in range(9)] for n in range(2)]
        for g in groups:
            for n, u in enumerate(fields):
                block = result[u, at(g), :]
                for d in range(9):
                    block = block - shifted[d, at(g), :] * gains[n][d]
                result[u, at(g), :] = block
        return mean

    gathered = tables[27]
    edge = jnp.logical_or(lane8 < 32, lane8 >= 96)
    for g in range(GROUPS):
        around[at(g), :] = jnp.where(edge, f_in[1, at(g), :], take(f_in[2, at(g), :], gathered))
    own = f_in.at[0]
    for g in groups:
        first_shifts[4, at(g), :] = own[at(g), :]
        for d in range(9):
            if d != 4:
                lanes = jnp.bitwise_and(tables[d], CELLS - 1)
                first_shifts[d, at(g), :] = jnp.where(
                    tables[d] >= CELLS, take(around[at(g), :], lanes), own_shifts[d, at(g), :]
                )
    observe(0, (own, around), (0, 9))

    for u in range(FIELDS):
        total = zero
        for g in groups:
            total = total + atm[u, at(g), :]
        mean = allsum(total) / MEM
        field_mean[u] = mean
        for g in groups:
            result[u, at(g), :] = atm[u, at(g), :] - mean


    def reduce_covariance(pair):
        for u in (2 * pair, 2 * pair + 1):
            for d in range(9):
                covariance[u, d] = allsum(covariance[u, d])

    def first_covariance(pair):
        fields = (2 * pair, 2 * pair + 1)
        if pair > 0:
            reduce_covariance(pair - 1)
        sums = [[zero] * 9, [zero] * 9]
        for g in groups:
            for n, u in enumerate(fields):
                block = result[u, at(g), :]
                for d in range(9):
                    sums[n][d] = sums[n][d] + first_shifts[d, at(g), :] * block
        for n, u in enumerate(fields):
            for d in range(9):
                covariance[u, d] = sums[n][d]
        shift_groups(9, other_shifts, own, around, groups[2 * pair : 2 * pair + 2])

    for pair in range(pairs):
        region(pair)(functools.partial(first_covariance, pair))
    reduce_covariance(pairs - 1)
    state[0, MEM:, :] = sst_step(0, own, own[MEM:, :], first_shifts, state.at[0])
    mean = shift(9, 4, own[MEM:, :], around[MEM:, :])
    state[1, MEM:, :] = sst_step(9, other_shifts.at[4], mean, other_shifts, state.at[1])
    observe(1, (state.at[0], state.at[1]), (18,))

    def first_update(pair):
        fields = (2 * pair, 2 * pair + 1)
        sums = [[covariance[u, d] for d in range(9)] for u in fields]
        mean = field_step(0, first_shifts, fields, sums)
        for n, u in enumerate(fields):
            field_mean[u] = mean[n]
        shift_groups(
            18, second_shifts, state.at[0], state.at[1], groups[2 * pair : 2 * pair + 2]
        )

    for pair in range(pairs):
        region(pairs + pair)(functools.partial(first_update, pair))
    mean = sst_step(18, state.at[0], state[0, MEM:, :], second_shifts, result.at[FIELDS])
    means[FIELDS] = mean[:1]
    sst_copy = pltpu.make_async_copy(result.at[FIELDS], anom_out.at[FIELDS], mean_sem.at[1])
    sst_copy.start()

    def field_copy(pair):
        part = pl.ds(2 * pair, 2)
        return pltpu.make_async_copy(result.at[part], anom_out.at[part], out_sem.at[pair])

    def second_batch(pair):
        fields = (2 * pair, 2 * pair + 1)
        sums = [[zero] * 9, [zero] * 9]
        for g in groups:
            for n, u in enumerate(fields):
                block = result[u, at(g), :]
                for d in range(9):
                    sums[n][d] = sums[n][d] + second_shifts[d, at(g), :] * block
        sums = [[allsum(x) for x in sums[n]] for n in range(2)]
        mean = field_step(18, second_shifts, fields, sums)
        for n, u in enumerate(fields):
            means[u] = mean[n][:1]
        field_copy(pair).start()

    for pair in range(pairs):
        region(2 * pairs + pair)(functools.partial(second_batch, pair))
    mean_copy = pltpu.make_async_copy(means, mean_out, mean_sem.at[0])
    mean_copy.start()
    sst_copy.wait()
    for pair in range(pairs):
        field_copy(pair).wait()
    mean_copy.wait()


def local(
    atm_members,
    ocean_members,
    remap_weights,
    pair_src,
    obs_cell,
    obs_value,
    obs_error,
    obs_live,
    obs_order,
):
    f32 = jnp.float32
    shifts, owners = build_tables()
    vmem = pl.BlockSpec(memory_space=pltpu.VMEM)
    hbm = pl.BlockSpec(memory_space=pltpu.HBM)
    dma = pltpu.SemaphoreType.DMA
    state, own_shifts, tables = pl.pallas_call(
        exchange_kernel,
        out_shape=(
            jax.ShapeDtypeStruct((3, ROWS, CELLS), f32),
            jax.ShapeDtypeStruct((9, MEM, CELLS), f32),
            jax.ShapeDtypeStruct((NB, 2, 4, OB, CELLS), f32),
        ),
        in_specs=[hbm] * 9,
        out_specs=(vmem, vmem, vmem),
        scratch_shapes=[
            pltpu.SMEM((1, K), jnp.int32),
            pltpu.VMEM((8, CELLS), jnp.int32),
            pltpu.VMEM((3, 1, OBS), jnp.int32),
            pltpu.VMEM((2, 1, OBS), f32),
            pltpu.VMEM((9, CHUNKS, MEM, CW), jnp.bfloat16),
            pltpu.VMEM((K, OCN_DEV, CELLS), jnp.bfloat16),
            pltpu.VMEM((MEM, CELLS), f32),
            pltpu.VMEM((CELLS, CELLS), f32),
            pltpu.VMEM((9, 8, CELLS), f32),
            pltpu.VMEM((2, 16, CELLS), f32),
            pltpu.VMEM((2, 24, CELLS), f32),
            pltpu.VMEM((2, 3, 16, CELLS), f32),
            pltpu.VMEM((2, 24, CELLS), f32),
            dma((CHUNKS + 8,)),
            dma((24,)),
            dma((9, CHUNKS)),
            dma((2,)),
            dma((2,)),
            dma((4,)),
            dma((9,)),
            dma((9,)),
            dma((9,)),
        ],
        compiler_params=pltpu.CompilerParams(
            collective_id=0, has_side_effects=True, vmem_limit_bytes=16 * 1024 * 1024
        ),
    )(
        *(
            pltpu.with_memory_space_constraint(x, pltpu.HBM)
            for x in (
                pair_src[0],
                ocean_members[0, 0],
                remap_weights[0, 0],
                obs_cell[0],
                obs_value[0],
                obs_error[0],
                obs_live[0],
                obs_order[0],
                jnp.asarray(owners),
            )
        )
    )
    mean, anomaly = pl.pallas_call(
        update_kernel,
        out_shape=(
            jax.ShapeDtypeStruct((COMP, 1, CELLS), f32),
            jax.ShapeDtypeStruct((COMP, MEM, CELLS), f32),
        ),
        in_specs=[vmem] * 5,
        out_specs=(hbm, hbm),
        scratch_shapes=[
            pltpu.VMEM((ROWS, CELLS), f32),
            pltpu.VMEM((2, ROWS, CELLS), f32),
            pltpu.VMEM((9, MEM, CELLS), f32),
            pltpu.VMEM((9, MEM, CELLS), f32),
            pltpu.VMEM((9, MEM, CELLS), f32),
            pltpu.VMEM((2, 27, 8, CELLS), f32),
            pltpu.VMEM((FIELDS, 9, 8, CELLS), f32),
            pltpu.VMEM((COMP, MEM, CELLS), f32),
            pltpu.VMEM((FIELDS, 8, CELLS), f32),
            pltpu.VMEM((COMP, 1, CELLS), f32),
            dma((FIELDS // 2,)),
            dma((2,)),
        ],
        compiler_params=pltpu.CompilerParams(vmem_limit_bytes=16 * 1024 * 1024),
    )(state, own_shifts, tables, jnp.asarray(shifts), jnp.transpose(atm_members[0, 0], (1, 0, 2)))
    return (mean.reshape(1, 1, COMP, CELLS), jnp.transpose(anomaly, (1, 0, 2))[None, None])


def solution(mesh):
    in_specs = (
        P("gx", "gy", None, None, None),
        P("gx", "gy", None, None),
        P("gx", "gy", None, None, None),
        P("gx", "gy", None),
        P("gx", "gy", None),
        P("gx", "gy", None),
        P("gx", "gy", None),
        P("gx", "gy", None),
        P("gx", "gy", None),
    )
    out_specs = (P("gx", "gy", None, None), P("gx", "gy", None, None, None))
    return jax.shard_map(local, mesh=mesh, in_specs=in_specs, out_specs=out_specs, check_vma=False)
```
